16 devices in a mesh: model: 2 (over z), data: 8 (over y, x, core).
Axes of the slice: x: 2, y: 2, z: 2, core: 2. Of those that a mesh axis runs over, the one named last changes fastest.
Arguments:
- tokens: bfloat16 [16384, 768], P('data')
- w_up: bfloat16 [768, 3072], P(None, 'model')
- w_down: bfloat16 [3072, 768], P('model')
- task_heads: bfloat16 [4, 768, 3], replicated
- labels: int32 [4, 16384], P(None, 'data')
Outputs:
- output 1: float32 [4], replicated
- output 2: float32 [768, 3072], P('data', 'model')
- output 3: float32 [3072, 768], P(('model', 'data'))
All inputs are finite; a program needn't handle non-finite values.
Results may differ from the reference program's by a relative error of at most 0.001.
Values are sent between devices in bfloat16 or wider.
A program may use at most 1 GiB of HBM per device.

```python
import jax
import jax.numpy as jnp
from jax import lax

HIDDEN = 768
FFN = 3072
CLASSES = 3
TASKS = 4
TOKENS = 16384
SEGMENT = 2048
BLOCK = 256
STEPS = 20


def setup_inputs(seed: int = 0) -> dict:
    key_list = jax.random.split(jax.random.key(seed), 12)
    n_seg = TOKENS // SEGMENT
    seg_shift = jax.random.normal(key_list[0], (n_seg, 1, HIDDEN), jnp.float32)
    x_body = jax.random.normal(key_list[1], (n_seg, SEGMENT, HIDDEN), jnp.float32)
    tokens = (x_body + 0.5 * seg_shift).reshape(TOKENS, HIDDEN).astype(jnp.bfloat16)
    w_up = (jax.random.normal(key_list[2], (HIDDEN, FFN), jnp.float32) * HIDDEN ** -0.5).astype(jnp.bfloat16)
    w_down = (jax.random.normal(key_list[3], (FFN, HIDDEN), jnp.float32) * FFN ** -0.5).astype(jnp.bfloat16)
    task_sign = jnp.where(jnp.arange(TASKS) % 2 == 0, 1.0, -1.0).astype(jnp.float32)
    head_base = jax.random.normal(key_list[4], (HIDDEN, CLASSES), jnp.float32)
    head_own = jax.random.normal(key_list[5], (TASKS, HIDDEN, CLASSES), jnp.float32)
    task_heads = ((0.8 * task_sign[:, None, None] * head_base[None] + 0.6 * head_own) * (1.5 * HIDDEN ** -0.5)).astype(jnp.bfloat16)
    seg_pref = jax.random.randint(key_list[6], (n_seg, 1), 0, CLASSES)
    keep_pref = jax.random.randint(key_list[7], (n_seg, SEGMENT), 0, 4)
    any_label = jax.random.randint(key_list[8], (n_seg, SEGMENT), 0, CLASSES)
    shared = jnp.where(keep_pref < 3, seg_pref, any_label).reshape(TOKENS)
    own_label = jax.random.randint(key_list[9], (TASKS, TOKENS), 0, CLASSES)
    keep_shared = jax.random.randint(key_list[10], (TASKS, TOKENS), 0, 4)
    labels = jnp.where(keep_shared < 3, shared[None, :], own_label).astype(jnp.int32)
    return {'tokens': tokens, 'w_up': w_up, 'w_down': w_down, 'task_heads': task_heads, 'labels': labels}


def simplex_weights(gram_mat):
    trace_scale = jnp.trace(gram_mat) / TASKS

    def eg_step(weights, unused):
        updated = weights * jnp.exp(-jnp.sum(gram_mat * weights[None, :], axis=1) / trace_scale)
        return updated / jnp.sum(updated), None

    start_w = jnp.full((TASKS,), 1.0 / TASKS, jnp.float32)
    weights, unused = lax.scan(eg_step, start_w, None, length=STEPS)
    return weights


def reference(tokens, w_up, w_down, task_heads, labels):
    n_blocks = TOKENS // BLOCK
    tok_blocks = tokens.reshape(n_blocks, BLOCK, HIDDEN)
    lab_blocks = labels.reshape(TASKS, n_blocks, BLOCK).transpose(1, 0, 2)
    heads_f = task_heads.astype(jnp.float32)
    down_f = w_down.astype(jnp.float32)

    def block_grads(grad_acc, block_in):
        tok_blk, lab_blk = block_in
        pre_act = jnp.dot(tok_blk, w_up, preferred_element_type=jnp.float32)
        act_val, gelu_slope = jax.jvp(jax.nn.gelu, (pre_act,), (jnp.ones_like(pre_act),))
        act_bf = act_val.astype(jnp.bfloat16)
        mlp_out = jnp.dot(act_bf, w_down, preferred_element_type=jnp.float32)
        trunk_out = (tok_blk.astype(jnp.float32) + mlp_out).astype(jnp.bfloat16)
        logits = jnp.einsum('bd,tdc->tbc', trunk_out.astype(jnp.float32), heads_f)
        class_prob = jax.nn.softmax(logits, axis=-1)
        onehot = jax.nn.one_hot(lab_blk, CLASSES, dtype=jnp.float32)
        dlogit = (class_prob - onehot) / TOKENS
        d_trunk = jnp.einsum('tbc,tdc->tbd', dlogit, heads_f).astype(jnp.bfloat16).astype(jnp.float32)
        g_down = jnp.einsum('bf,tbd->tfd', act_bf.astype(jnp.float32), d_trunk)
        d_act = jnp.einsum('tbd,fd->tbf', d_trunk, down_f)
        d_pre = (d_act * gelu_slope[None]).astype(jnp.bfloat16).astype(jnp.float32)
        g_up = jnp.einsum('bd,tbf->tdf', tok_blk.astype(jnp.float32), d_pre)
        return (grad_acc[0] + g_up, grad_acc[1] + g_down), None

    zero_acc = (jnp.zeros((TASKS, HIDDEN, FFN), jnp.float32), jnp.zeros((TASKS, FFN, HIDDEN), jnp.float32))
    (g_up, g_down), unused = lax.scan(block_grads, zero_acc, (tok_blocks, lab_blocks))
    gram_mat = jnp.einsum('tij,sij->ts', g_up, g_up) + jnp.einsum('tij,sij->ts', g_down, g_down)
    task_weights = simplex_weights(gram_mat)
    grad_up = jnp.einsum('t,tij->ij', task_weights, g_up)
    grad_down = jnp.einsum('t,tij->ij', task_weights, g_down)
    return task_weights, grad_up, grad_down
```

```python
import functools

import jax
import jax.numpy as jnp
from jax import lax
from jax.experimental import pallas as pl
from jax.experimental.pallas import tpu as pltpu
from jax.sharding import PartitionSpec as P

STEPS = 20
MESH = pl.DeviceIdType.MESH
F32 = jnp.float32
BF16 = jnp.bfloat16
C0 = 0.7978845608028654
C1 = 0.044715
N_DATA = 8
N_TASK = 4
N_CLASS = 3
VMEM_LIMIT = 62 * 1024 * 1024


def gelu_only(a):
    return a * (0.5 + 0.5 * jnp.tanh(a * (C0 + (C0 * C1) * (a * a))))


def gelu_both(a):
    a2 = a * a
    t = jnp.tanh(a * (C0 + (C0 * C1) * a2))
    h = 0.5 + 0.5 * t
    slope = h + (0.5 * a) * (1.0 - t * t) * (C0 + (3.0 * C0 * C1) * a2)
    return a * h, slope


def nt_dot(a, b):
    return lax.dot_general(a, b, (((1,), (1,)), ((), ())), preferred_element_type=F32)


def nn_dot(a, b):
    return jnp.dot(a, b, preferred_element_type=F32)


def part_kernel(x_ref, w1_ref, w2_ref, out_ref):
    act = gelu_only(nn_dot(x_ref[...], w1_ref[...])).astype(BF16)
    out_ref[...] = nn_dot(act, w2_ref[...])


def part_call(x_half, w1, w2):
    rows, dim = x_half.shape
    ffn = w1.shape[1]
    blk = 256
    return pl.pallas_call(
        part_kernel,
        grid=(rows // blk,),
        out_shape=jax.ShapeDtypeStruct((rows, dim), F32),
        in_specs=[pl.BlockSpec((blk, dim), lambda i: (i, 0)),
                  pl.BlockSpec((dim, ffn), lambda i: (0, 0)),
                  pl.BlockSpec((ffn, dim), lambda i: (0, 0))],
        out_specs=pl.BlockSpec((blk, dim), lambda i: (i, 0)),
        compiler_params=pltpu.CompilerParams(vmem_limit_bytes=VMEM_LIMIT),
        cost_estimate=pl.CostEstimate(flops=4 * rows * dim * ffn, bytes_accessed=12_000_000, transcendentals=0),
    )(x_half, w1, w2)


def err_kernel(n_total, x_ref, w1_ref, w2_ref, part_ref, lab_ref, head_ref, out_ref, own_ref, send_sem, recv_sem, loc_sem):
    i = pl.program_id(0)
    blk = x_ref.shape[0]
    m = lax.axis_index('model')
    d = lax.axis_index('data')
    offs = [(dz, dr) for dz in (0, 1) for dr in range(4) if dz or dr]

    @pl.when(i == 0)
    def _():
        barrier = pltpu.get_barrier_semaphore()
        for dz, dr in offs:
            dev = (lax.rem(m + dz, 2), xor_data(d, dr))
            pl.semaphore_signal(barrier, inc=1, device_id=dev, device_id_type=MESH)
        pl.semaphore_wait(barrier, len(offs))

    x = x_ref[...]
    act = gelu_only(nn_dot(x, w1_ref[...])).astype(BF16)
    mlp = part_ref[...] + nn_dot(act, w2_ref[...])
    z = (x.astype(F32) + mlp).astype(BF16)
    logits = nt_dot(head_ref[...], z)
    lg = [logits[8 * c:8 * c + 8, :] for c in range(N_CLASS)]
    top = jnp.maximum(jnp.maximum(lg[0], lg[1]), lg[2])
    ex = [jnp.exp(v - top) for v in lg]
    tot = ex[0] + ex[1] + ex[2]
    lab = lab_ref[...]
    col = pl.ds(pl.multiple_of(i * blk, blk), blk)
    errs = []
    for c in range(N_CLASS):
        hot = jnp.where(lab == c, 1.0, 0.0)
        errs.append((ex[c] / tot - hot) * (1.0 / n_total))
    for c in range(N_CLASS):
        own_ref[8 * c:8 * c + 8, col] = errs[c]

    @pl.when(i == pl.num_programs(0) - 1)
    def _():
        loc = pltpu.make_async_copy(own_ref, out_ref.at[0, m], loc_sem)
        loc.start()
        copies = []
        for k, (dz, dr) in enumerate(offs):
            dev = (lax.rem(m + dz, 2), xor_data(d, dr))
            copies.append(pltpu.make_async_remote_copy(
                own_ref, out_ref.at[dr, m], send_sem.at[k], recv_sem.at[k], device_id=dev, device_id_type=MESH))
            copies[-1].start()
        for cp in copies:
            cp.wait()
        loc.wait()


def xor_data(d, dr):
    core = lax.rem(d, 2)
    x = lax.rem(d // 2, 2)
    y = d // 4
    return (lax.rem(y + dr // 2, 2) * 2 + lax.rem(x + dr % 2, 2)) * 2 + core


def err_call(n_total, x_half, w1, w2, part, lab8, heads24):
    rows, dim = x_half.shape
    ffn = w1.shape[1]
    blk = 256
    return pl.pallas_call(
        functools.partial(err_kernel, n_total),
        grid=(rows // blk,),
        out_shape=jax.ShapeDtypeStruct((4, 2, 24, rows), F32),
        in_specs=[pl.BlockSpec((blk, dim), lambda i: (i, 0)),
                  pl.BlockSpec((dim, ffn), lambda i: (0, 0)),
                  pl.BlockSpec((ffn, dim), lambda i: (0, 0)),
                  pl.BlockSpec((blk, dim), lambda i: (i, 0)),
                  pl.BlockSpec((8, blk), lambda i: (0, i)),
                  pl.BlockSpec((24, dim), lambda i: (0, 0))],
        out_specs=pl.BlockSpec(memory_space=pl.ANY),
        scratch_shapes=[pltpu.VMEM((24, rows), F32),
                        pltpu.SemaphoreType.DMA((7,)), pltpu.SemaphoreType.DMA((7,)), pltpu.SemaphoreType.DMA],
        compiler_params=pltpu.CompilerParams(vmem_limit_bytes=VMEM_LIMIT, collective_id=0, has_side_effects=True),
        cost_estimate=pl.CostEstimate(flops=4 * rows * dim * ffn, bytes_accessed=12_000_000, transcendentals=0),
    )(x_half, w1, w2, part, lab8, heads24)


def grad_body(x_ref, e_ref, w1t_ref, w2s_ref, hb_ref, g1_ref, g2_ref, dz_ref, da_ref, ut_ref, sl_ref, first):
    blk, dim = x_ref.shape
    sl = w1t_ref.shape[0]
    pre = nt_dot(w1t_ref[...], x_ref[...])
    act, slope = gelu_both(pre)
    ut_ref[...] = act.astype(BF16)
    sl_ref[...] = slope
    rows = 32
    for t in range(N_TASK):
        slot = t % 2
        es = [[e_ref[8 * c + t:8 * c + t + 1, 128 * j:128 * j + 128] for j in range(blk // 128)] for c in range(N_CLASS)]
        for r0 in range(0, dim, rows):
            h = [hb_ref[N_CLASS * t + c, r0:r0 + rows, :] for c in range(N_CLASS)]
            for j in range(blk // 128):
                val = h[0] * es[0][j] + h[1] * es[1][j] + h[2] * es[2][j]
                dz_ref[slot, r0:r0 + rows, 128 * j:128 * j + 128] = val.astype(BF16)
        da = nn_dot(w2s_ref[...], dz_ref[slot])
        da_ref[slot] = (da * sl_ref[...]).astype(BF16)
        g2 = nt_dot(ut_ref[...], dz_ref[slot])
        g1 = nn_dot(da_ref[slot], x_ref[...])
        out = pl.ds(t * sl, sl)
        if first:
            g2_ref[out, :] = g2
            g1_ref[out, :] = g1
        else:
            g2_ref[out, :] += g2
            g1_ref[out, :] += g1


def grad_kernel(has_acc, x_ref, e_ref, w1t_ref, w2s_ref, hb_ref, *rest):
    if has_acc:
        g1_in, g2_in, g1_ref, g2_ref, dz_ref, da_ref, ut_ref, sl_ref = rest
    else:
        g1_ref, g2_ref, dz_ref, da_ref, ut_ref, sl_ref = rest

    @pl.when(pl.program_id(0) == 0)
    def _():
        if has_acc:
            g1_ref[...] = g1_in[...]
            g2_ref[...] = g2_in[...]
        else:
            g1_ref[...] = jnp.zeros_like(g1_ref)
            g2_ref[...] = jnp.zeros_like(g2_ref)

    grad_body(x_ref, e_ref.at[0, 0], w1t_ref, w2s_ref, hb_ref, g1_ref, g2_ref, dz_ref, da_ref, ut_ref, sl_ref, False)


def grad_call(x_set, errs, rel, w1t, w2s, hb, acc):
    rows, dim = x_set.shape
    sl = w1t.shape[0]
    blk = 512
    per = errs.shape[3] // blk
    acc_spec = pl.BlockSpec((N_TASK * sl, dim), lambda i: (0, 0))
    acc_shape = jax.ShapeDtypeStruct((N_TASK * sl, dim), F32)
    in_specs = [pl.BlockSpec((blk, dim), lambda i: (i, 0)),
                pl.BlockSpec((1, 1, 24, blk), lambda i: (rel, i // per, 0, lax.rem(i, per))),
                pl.BlockSpec((sl, dim), lambda i: (0, 0)),
                pl.BlockSpec((sl, dim), lambda i: (0, 0)),
                pl.BlockSpec(hb.shape, lambda i: (0, 0, 0))]
    args = [x_set, errs, w1t, w2s, hb]
    if acc is not None:
        in_specs += [acc_spec, acc_spec]
        args += list(acc)
    return pl.pallas_call(
        functools.partial(grad_kernel, acc is not None),
        grid=(rows // blk,),
        out_shape=[acc_shape, acc_shape],
        in_specs=in_specs,
        out_specs=[acc_spec, acc_spec],
        scratch_shapes=[pltpu.VMEM((2, dim, blk), BF16), pltpu.VMEM((2, sl, blk), BF16),
                        pltpu.VMEM((sl, blk), BF16), pltpu.VMEM((sl, blk), F32)],
        compiler_params=pltpu.CompilerParams(vmem_limit_bytes=VMEM_LIMIT),
        cost_estimate=pl.CostEstimate(flops=26 * rows * dim * sl, bytes_accessed=30_000_000, transcendentals=0),
    )(*args)


def tail_kernel(g1_ref, g2_ref, wts_ref, out1_ref, out2_ref, rx1, rx2, gr_own, gr_all, tr_ref, rx_g1,
                half_send, half_recv, gram_send, gram_recv, out_send, out_recv, loc_sem):
    m = lax.axis_index('model')
    d = lax.axis_index('data')
    core = lax.rem(d, 2)
    n_data = N_DATA
    half = rx1.shape[1]
    sl = 2 * half
    dim = g1_ref.shape[1]
    me = m * n_data + d

    barrier = pltpu.get_barrier_semaphore()
    for k in range(1, 2 * n_data):
        p = lax.rem(me + k, 2 * n_data)
        pl.semaphore_signal(barrier, inc=1, device_id=(p // n_data, lax.rem(p, n_data)), device_id_type=MESH)
    pl.semaphore_wait(barrier, 2 * n_data - 1)

    peer = (m, d + 1 - 2 * core)
    keep = pl.multiple_of(core * half, half)
    give = pl.multiple_of((1 - core) * half, half)
    copies = []
    for a, (src, dst) in enumerate(((g1_ref, rx1), (g2_ref, rx2))):
        for t in range(N_TASK):
            copies.append(pltpu.make_async_remote_copy(
                src.at[pl.ds(t * sl + give, half), :], dst.at[t], half_send.at[a, t], half_recv.at[a, t],
                device_id=peer, device_id_type=MESH))
            copies[-1].start()
    pairs = [(i, j) for i in range(N_TASK) for j in range(i, N_TASK)]
    acc = tuple(jnp.zeros((8, 128), F32) for _ in pairs)
    for a, (src, dst) in enumerate(((g1_ref, rx1), (g2_ref, rx2))):
        for cp in copies[a * N_TASK:(a + 1) * N_TASK]:
            cp.wait_recv()

        def fold(r, acc):
            row = pl.multiple_of(r * 8, 8)
            acc = list(acc)
            for l in range(0, dim, 128):
                gs = []
                for t in range(N_TASK):
                    v = dst[t, pl.ds(row, 8), l:l + 128] + src[pl.ds(pl.multiple_of(t * sl + keep + row, 8), 8), l:l + 128]
                    dst[t, pl.ds(row, 8), l:l + 128] = v
                    gs.append(v)
                for q, (i, j) in enumerate(pairs):
                    acc[q] = acc[q] + gs[i] * gs[j]
            return tuple(acc)

        acc = lax.fori_loop(0, half // 8, fold, acc)
    for cp in copies:
        cp.wait_send()
    gr_own[...] = jnp.zeros_like(gr_own)
    for q in range(len(pairs)):
        gr_own[q:q + 1, :] = jnp.sum(acc[q], axis=0, keepdims=True)
    loc = pltpu.make_async_copy(gr_own, gr_all.at[me], loc_sem)
    loc.start()
    gcopies = []
    for k in range(1, 2 * n_data):
        p = lax.rem(me + k, 2 * n_data)
        gcopies.append(pltpu.make_async_remote_copy(
            gr_own, gr_all.at[me], gram_send.at[k - 1], gram_recv.at[k - 1],
            device_id=(p // n_data, lax.rem(p, n_data)), device_id_type=MESH))
        gcopies[-1].start()
    for cp in gcopies:
        cp.wait()
    loc.wait()
    tot = gr_all[0]
    for k in range(1, 2 * n_data):
        tot = tot + gr_all[k]
    sums = jnp.broadcast_to(jnp.sum(tot, axis=1, keepdims=True), tot.shape)
    gram = {}
    for q, (i, j) in enumerate(pairs):
        gram[i, j] = gram[j, i] = sums[q:q + 1, :]
    scale = (gram[0, 0] + gram[1, 1] + gram[2, 2] + gram[3, 3]) / N_TASK

    def eg_step(k, w):
        up = []
        for i in range(N_TASK):
            mv = gram[i, 0] * w[0] + gram[i, 1] * w[1] + gram[i, 2] * w[2] + gram[i, 3] * w[3]
            up.append(w[i] * jnp.exp(-mv / scale))
        s = up[0] + up[1] + up[2] + up[3]
        return tuple(u / s for u in up)

    w = lax.fori_loop(0, STEPS, eg_step, tuple(jnp.full((1, 128), 1.0 / N_TASK, F32) for _ in range(N_TASK)))
    wts_ref[...] = jnp.zeros_like(wts_ref)
    for t in range(N_TASK):
        wts_ref[t:t + 1, :] = w[t]
    w1 = [jnp.broadcast_to(v, (half, 128)) for v in w]
    for l in range(0, dim, 128):
        v = w1[0] * rx1[0, :, l:l + 128]
        for t in range(1, N_TASK):
            v = v + w1[t] * rx1[t, :, l:l + 128]
        tr_ref[l:l + 128, 0:half] = v.T
    per = dim // n_data
    ocopies = []
    for k in range(1, n_data):
        p = lax.rem(d + k, n_data)
        ocopies.append(pltpu.make_async_remote_copy(
            tr_ref.at[pl.ds(pl.multiple_of(p * per, per), per), :], rx_g1.at[d], out_send.at[k - 1], out_recv.at[k - 1],
            device_id=(m, p), device_id_type=MESH))
        ocopies[-1].start()
    loc = pltpu.make_async_copy(tr_ref.at[pl.ds(pl.multiple_of(d * per, per), per), :], rx_g1.at[d], loc_sem)
    loc.start()
    for l in range(0, dim, 128):
        v = w1[0] * rx2[0, :, l:l + 128]
        for t in range(1, N_TASK):
            v = v + w1[t] * rx2[t, :, l:l + 128]
        out2_ref[:, l:l + 128] = v
    loc.wait()
    for cp in ocopies:
        cp.wait()
    for k in range(n_data):
        out1_ref[:, k * half:(k + 1) * half] = rx_g1[k, :, 0:half]


def tail_call(g1, g2):
    rows, dim = g1.shape
    sl = rows // N_TASK
    half = sl // 2
    per = dim // N_DATA
    n_dev = 2 * N_DATA
    vm = pl.BlockSpec(memory_space=pltpu.VMEM)
    return pl.pallas_call(
        tail_kernel,
        out_shape=[jax.ShapeDtypeStruct((8, 128), F32), jax.ShapeDtypeStruct((per, half * N_DATA), F32),
                   jax.ShapeDtypeStruct((half, dim), F32)],
        in_specs=[vm, vm],
        out_specs=[vm, vm, vm],
        scratch_shapes=[pltpu.VMEM((N_TASK, half, dim), F32), pltpu.VMEM((N_TASK, half, dim), F32),
                        pltpu.VMEM((16, 128), F32), pltpu.VMEM((n_dev, 16, 128), F32),
                        pltpu.VMEM((dim, 256), F32), pltpu.VMEM((N_DATA, per, 256), F32),
                        pltpu.SemaphoreType.DMA((2, N_TASK)), pltpu.SemaphoreType.DMA((2, N_TASK)),
                        pltpu.SemaphoreType.DMA((n_dev - 1,)), pltpu.SemaphoreType.DMA((n_dev - 1,)),
                        pltpu.SemaphoreType.DMA((N_DATA - 1,)), pltpu.SemaphoreType.DMA((N_DATA - 1,)),
                        pltpu.SemaphoreType.DMA],
        compiler_params=pltpu.CompilerParams(vmem_limit_bytes=VMEM_LIMIT, collective_id=1, has_side_effects=True),
    )(g1, g2)


def swap(v, bit):
    return lax.ppermute(v, 'data', [(i, i ^ bit) for i in range(N_DATA)])


def solution(mesh):
    n_data = mesh.shape['data']

    def local_step(tokens, w_up, w_down, task_heads, labels):
        m = lax.axis_index('model')
        d = lax.axis_index('data')
        n_loc, dim = tokens.shape
        n_total = n_loc * n_data
        n_half = n_loc // 2
        wide = w_up.shape[1]
        sl = 2 * wide // n_data
        flip = [(0, 1), (1, 0)]
        p1 = dim // n_data
        p2 = wide // n_data
        w1_part = lax.ppermute(lax.dynamic_slice_in_dim(w_up, d * p1, p1, 0), 'model', flip)
        w2_part = lax.ppermute(lax.dynamic_slice_in_dim(w_down, d * p2, p2, 0), 'model', flip)
        w1_far = lax.all_gather(w1_part, 'data', axis=0, tiled=True)
        w2_far = lax.all_gather(w2_part, 'data', axis=0, tiled=True)
        x_a = swap(tokens, 2)
        x_b = swap(tokens, 4)
        x_c0 = swap(x_a[:n_half], 4)
        x_c1 = swap(x_b[n_half:], 2)

        heads_t = task_heads.transpose(2, 0, 1)
        heads24 = jnp.pad(heads_t, ((0, 0), (0, 4), (0, 0))).reshape(24, dim)
        hb = jnp.broadcast_to(task_heads.astype(F32).transpose(0, 2, 1).reshape(12, dim, 1), (12, dim, 128))
        chip = d // 2
        w1t = lax.dynamic_slice_in_dim(w_up, chip * sl, sl, 1).T
        w2s = lax.dynamic_slice_in_dim(w_down, chip * sl, sl, 0)
        x_half = lax.dynamic_slice_in_dim(tokens, m * n_half, n_half, 0)
        lab8 = jnp.pad(lax.dynamic_slice_in_dim(labels, m * n_half, n_half, 1), ((0, 4), (0, 0)))

        part = part_call(x_half, w_up, w_down)
        errs = err_call(n_total, x_half, w1_far, w2_far, part, lab8, heads24)
        acc = grad_call(tokens, errs, 0, w1t, w2s, hb, None)
        acc = grad_call(x_a, errs, 1, w1t, w2s, hb, acc)
        acc = grad_call(x_b, errs, 2, w1t, w2s, hb, acc)
        x_c = jnp.concatenate([x_c0, x_c1], axis=0)
        acc = grad_call(x_c, errs, 3, w1t, w2s, hb, acc)
        wts, grad_up, grad_down = tail_call(*acc)
        return wts[:N_TASK, 0], grad_up, grad_down

    return jax.shard_map(
        local_step, mesh=mesh,
        in_specs=(P('data', None), P(None, 'model'), P('model', None), P(None, None, None), P(None, 'data')),
        out_specs=(P(None), P('data', 'model'), P(('model', 'data'), None)),
        check_vma=False)
```

```python
import functools

import jax
import jax.numpy as jnp
from jax import lax
from jax.experimental import pallas as pl
from jax.experimental.pallas import tpu as pltpu
from jax.sharding import PartitionSpec as P

STEPS = 20
MESH = pl.DeviceIdType.MESH
F32 = jnp.float32
BF16 = jnp.bfloat16
C0 = 0.7978845608028654
C1 = 0.044715
N_DATA = 8
N_DEV = 16
N_TASK = 4
N_CLASS = 3
BLK = 512
VMEM_LIMIT = 63 * 1024 * 1024


def gelu_only(a):
    return a * (0.5 + 0.5 * jnp.tanh(a * (C0 + (C0 * C1) * (a * a))))


def gelu_both(a):
    a2 = a * a
    t = jnp.tanh(a * (C0 + (C0 * C1) * a2))
    h = 0.5 + 0.5 * t
    slope = h + (0.5 * a) * (1.0 - t * t) * (C0 + (3.0 * C0 * C1) * a2)
    return a * h, slope


def nt_dot(a, b):
    return lax.dot_general(a, b, (((1,), (1,)), ((), ())), preferred_element_type=F32)


def nn_dot(a, b):
    return jnp.dot(a, b, preferred_element_type=F32)


def xor_data(d, dr):
    core = lax.rem(d, 2)
    x = lax.rem(d // 2, 2)
    y = d // 4
    return (lax.rem(y + dr // 2, 2) * 2 + lax.rem(x + dr % 2, 2)) * 2 + core


def dz_part(e_ref, s, t, hb_ref, dz):
    dim, blk = dz.shape
    rows = 32
    es = [[e_ref[s, N_TASK * c + t:N_TASK * c + t + 1, 128 * j:128 * j + 128] for j in range(blk // 128)]
          for c in range(N_CLASS)]
    for r0 in range(0, dim, rows):
        h = [hb_ref[N_CLASS * t + c, r0:r0 + rows, :] for c in range(N_CLASS)]
        for j in range(blk // 128):
            val = h[0] * es[0][j] + h[1] * es[1][j] + h[2] * es[2][j]
            dz[r0:r0 + rows, 128 * j:128 * j + 128] = val.astype(BF16)


def act_cols(x_ref, s, w1t_ref, ut, sl, lo, hi):
    act, slope = gelu_both(nt_dot(w1t_ref[...], x_ref[s, lo:hi, :]))
    ut[:, lo:hi] = act.astype(BF16)
    sl[:, lo:hi] = slope


def mega_kernel(n_total, x_hbm, w1_hbm, w2_hbm, heads_ref, lab_ref, wts_ref, out1_ref, out2_ref,
                x_all, e_all, w1v, w2v, w1f, w2f, w1t, w2s, hb, h24, part, act_far, g1, g2, rx1, rx2,
                dz0, dz1, da0, da1, ut0, ut1, sl0, sl1, gr_own, gr_all, tr_ref, rx_g1,
                ssem, rsem, lsem):
    m = lax.axis_index('model')
    d = lax.axis_index('data')
    core = lax.rem(d, 2)
    chip = d // 2
    me = m * N_DATA + d
    dim = x_all.shape[2]
    wide = w1v.shape[1]
    sl = w1t.shape[0]
    half = sl // 2
    p1 = dim // N_DATA
    p2 = wide // N_DATA

    lcopy = [pltpu.make_async_copy(x_hbm.at[pl.ds(pl.multiple_of((2 * m + k) * BLK, BLK), BLK), :], x_all.at[k], lsem.at[k])
             for k in range(2)]
    lcopy += [pltpu.make_async_copy(w1_hbm, w1v, lsem.at[2]), pltpu.make_async_copy(w2_hbm, w2v, lsem.at[3])]
    lcopy += [pltpu.make_async_copy(x_hbm.at[pl.ds(pl.multiple_of((2 - 2 * m + k) * BLK, BLK), BLK), :], x_all.at[2 + k],
                                    lsem.at[4 + k]) for k in range(2)]
    for cp in lcopy:
        cp.start()

    barrier = pltpu.get_barrier_semaphore()
    for k in range(1, N_DEV):
        p = lax.rem(me + k, N_DEV)
        pl.semaphore_signal(barrier, inc=1, device_id=(p // N_DATA, lax.rem(p, N_DATA)), device_id_type=MESH)
    pl.semaphore_wait(barrier, N_DEV - 1)

    twin = (1 - m, d)
    peer = (m, d + 1 - 2 * core)
    nb_x = (m, xor_data(d, 1))
    nb_y = (m, xor_data(d, 2))

    table = {}

    def rcopy(name, src, dst, dev):
        if name not in table:
            table[name] = len(table)
        k = table[name]
        return pltpu.make_async_remote_copy(src, dst, ssem.at[k], rsem.at[k], device_id=dev, device_id_type=MESH)

    def w1_rows(dr):
        return w1f.at[pl.ds(pl.multiple_of(xor_data(d, dr) * p1, p1), p1), :]

    def w2_rows(dr):
        return w2f.at[pl.ds(pl.multiple_of(xor_data(d, dr) * p2, p2), p2), :]

    rows_of = {1: w1_rows, 2: w2_rows}

    def w_copy(w, name, dr, dev):
        return rcopy(f'w{w}{name}', rows_of[w](dr), rows_of[w](dr), dev)

    wt = {1: rcopy('w1t', w1_hbm.at[pl.ds(pl.multiple_of(d * p1, p1), p1), :], w1_rows(0), twin),
          2: rcopy('w2t', w2_hbm.at[pl.ds(pl.multiple_of(d * p2, p2), p2), :], w2_rows(0), twin)}
    w_own = {(w, n): w_copy(w, 'own' + n, 0, dev) for w in (1, 2) for n, dev in (('p', peer), ('x', nb_x), ('y', nb_y))}
    w_peer = {(w, dr): w_copy(w, f'peer{dr}', dr, peer) for w in (1, 2) for dr in (1, 2, 3)}
    w_fwd = {1: w_copy(1, 'fwd', 1, nb_y), 2: w_copy(2, 'fwd', 2, nb_x)}

    def own_block(b, lo, n):
        return x_hbm.at[pl.ds(pl.multiple_of(b * BLK + lo, BLK // 2), n), :]

    hb2 = BLK // 2
    first_x = [rcopy(f'fx{h}', own_block(3 * m, h * hb2, hb2), x_all.at[4, pl.ds(h * hb2, hb2), :], nb_x) for h in (0, 1)]
    first_y = [rcopy(f'fy{h}', own_block(1 + m, h * hb2, hb2), x_all.at[5, pl.ds(h * hb2, hb2), :], nb_y) for h in (0, 1)]
    more_x = [rcopy(f'mx{b}', own_block(b, 0, BLK), x_all.at[s], nb_x) for b, s in ((1, 10), (2, 13))]
    more_y = [rcopy(f'my{b}', own_block(b, 0, BLK), x_all.at[s], nb_y) for b, s in ((0, 11), (3, 14))]
    fwd_x = rcopy('dx', x_all.at[5], x_all.at[8], nb_x)
    fwd_y = rcopy('dy', x_all.at[4], x_all.at[9], nb_y)
    z_x = [rcopy(f'zx{h}', x_all.at[4, pl.ds(h * hb2, hb2), :], x_all.at[6, pl.ds(h * hb2, hb2), :], twin) for h in (0, 1)]
    z_y = [rcopy(f'zy{h}', x_all.at[5, pl.ds(h * hb2, hb2), :], x_all.at[7, pl.ds(h * hb2, hb2), :], twin) for h in (0, 1)]
    z_d = [rcopy('zd8', x_all.at[8], x_all.at[12], twin), rcopy('zd9', x_all.at[9], x_all.at[15], twin)]

    k_out, k_in = m, 1 - m
    e_twin = [rcopy(f'et{k}', e_all.at[k], e_all.at[2 + k], twin) for k in range(2)]
    e_rest = []
    for dz in (0, 1):
        for dr in (1, 2, 3):
            dev = (lax.rem(m + dz, 2), xor_data(d, dr))
            s_out, s_in = {1: (4 + 2 * dz, 10 + 3 * m), 2: (11 + 3 * m, 5 + 2 * dz), 3: (9 + 6 * dz, 8 + 4 * dz)}[dr]
            e_rest.append(rcopy(f'eo{dz}{dr}', e_all.at[k_out], e_all.at[s_out], dev))
            e_rest.append(rcopy(f'ei{dz}{dr}', e_all.at[k_in], e_all.at[s_in], dev))

    wt[1].start()
    first_x[0].start()
    first_y[0].start()
    wt[2].start()

    h24[...] = jnp.zeros_like(h24)
    for t in range(N_TASK):
        h = heads_ref[t].astype(F32)
        for c in range(N_CLASS):
            hb[N_CLASS * t + c] = jnp.broadcast_to(h[:, c:c + 1], (dim, 128))
        ht = h.T
        for c in range(N_CLASS):
            h24[8 * c + t:8 * c + t + 1, :] = ht[c:c + 1, :]
    for k in range(4):
        lcopy[k].wait()
    off = pl.multiple_of(chip * sl, sl)
    w1t[...] = w1v[:, pl.ds(off, sl)].T
    w2s[...] = w2v[pl.ds(off, sl), :]

    fc = wide // 3

    def part_block(k):
        x = x_all[k]
        acc = None
        for f in range(0, wide, fc):
            u = gelu_only(nn_dot(x, w1v[:, f:f + fc])).astype(BF16)
            y = nn_dot(u, w2v[f:f + fc, :])
            acc = y if acc is None else acc + y
        part[k] = acc

    part_block(0)
    wt[1].wait_recv()
    for n in 'pxy':
        w_own[1, n].start()
    part_block(1)
    wt[2].wait_recv()
    for n in 'pxy':
        w_own[2, n].start()
    first_x[0].wait_recv()
    z_x[0].start()
    first_y[0].wait_recv()
    z_y[0].start()
    w_own[1, 'x'].wait_recv()
    w_fwd[1].start()
    w_peer[1, 1].start()
    w_own[1, 'y'].wait_recv()
    w_peer[1, 2].start()
    first_y[1].start()
    w_own[2, 'y'].wait_recv()
    w_fwd[2].start()
    w_peer[2, 2].start()
    first_x[1].start()
    w_own[2, 'x'].wait_recv()
    w_peer[2, 1].start()
    w_fwd[1].wait_recv()
    w_peer[1, 3].start()
    w_own[1, 'p'].wait_recv()
    for dr in (1, 2, 3):
        w_peer[1, dr].wait_recv()
    for k in range(2):
        x = x_all[k]
        for f in range(0, wide, fc):
            act_far[k, :, f:f + fc] = gelu_only(nn_dot(x, w1f[:, f:f + fc])).astype(BF16)
    w_fwd[2].wait_recv()
    w_peer[2, 3].start()
    w_own[2, 'p'].wait_recv()
    for dr in (1, 2, 3):
        w_peer[2, dr].wait_recv()
    heads24 = h24[...].astype(BF16)
    for k in range(2):
        mlp = part[k] + nn_dot(act_far[k], w2f[...])
        z = (x_all[k].astype(F32) + mlp).astype(BF16)
        logits = nt_dot(heads24, z)
        lg = [logits[8 * c:8 * c + N_TASK, :] for c in range(N_CLASS)]
        top = jnp.maximum(jnp.maximum(lg[0], lg[1]), lg[2])
        ex = [jnp.exp(v - top) for v in lg]
        tot = ex[0] + ex[1] + ex[2]
        lab = lab_ref[:, pl.ds(pl.multiple_of((2 * m + k) * BLK, BLK), BLK)]
        for c in range(N_CLASS):
            hot = jnp.where(lab == c, 1.0, 0.0)
            e_all[k, N_TASK * c:N_TASK * c + N_TASK, :] = (ex[c] / tot - hot) * (1.0 / n_total)
        e_all[k, 12:16, :] = jnp.zeros((4, BLK), F32)
    for cp in e_twin + e_rest:
        cp.start()

    dzs, das, uts, sls = (dz0, dz1), (da0, da1), (ut0, ut1), (sl0, sl1)
    n_blk = x_all.shape[0]
    g1[...] = jnp.zeros_like(g1)
    g2[...] = jnp.zeros_like(g2)
    for lo in range(0, BLK, 256):
        act_cols(x_all, 0, w1t, ut0, sl0, lo, lo + 256)
    dz_part(e_all, 0, 0, hb, dz0)

    def links_1():
        first_x[1].wait_recv()
        first_y[1].wait_recv()
        for cp in (fwd_x, fwd_y, z_x[1], z_y[1], more_x[0], more_y[0], more_x[1], more_y[1]):
            cp.start()

    def links_2():
        for cp in (fwd_x, fwd_y):
            cp.wait_recv()
        for cp in z_d:
            cp.start()

    def arrive(*cps):
        def go():
            for cp in cps:
                cp.wait_recv()
        return go

    actions = {1: [arrive(*e_twin)], 2: [links_1],
               3: [arrive(*e_rest)], 5: [arrive(*z_x)], 6: [arrive(*z_y), links_2],
               9: [arrive(more_x[0])], 10: [arrive(more_y[0])], 11: [arrive(z_d[0])], 12: [arrive(more_x[1])],
               13: [arrive(more_y[1])], 14: [arrive(z_d[1])]}
    lcopy[4].wait()
    lcopy[5].wait()

    def step(p, q):
        s = 2 * p + q
        for k, acts in actions.items():
            if k % 2 == q:
                @pl.when(p == k // 2)
                def _():
                    for act in acts:
                        act()
        nxt = jnp.minimum(s + 1, n_blk - 1)
        ut, slp = uts[q], sls[q]
        for t in range(N_TASK):
            dz, da = dzs[t % 2], das[t % 2]
            sn, tn = (s, t + 1) if t < N_TASK - 1 else (nxt, 0)
            rows = slice(t * sl, (t + 1) * sl)
            da[...] = (nn_dot(w2s[...], dz[...]) * slp[...]).astype(BF16)
            dz_part(e_all, sn, tn, hb, dzs[(t + 1) % 2])
            if t < 2:
                act_cols(x_all, nxt, w1t, uts[1 - q], sls[1 - q], 256 * t, 256 * t + 256)
            g2[rows, :] += nt_dot(ut[...], dz[...])
            g1[rows, :] += nn_dot(da[...], x_all[s])

    def pair(p, c):
        step(p, 0)
        step(p, 1)
        return c

    lax.fori_loop(0, n_blk // 2, pair, 0)

    keep = pl.multiple_of(core * half, half)
    give = pl.multiple_of((1 - core) * half, half)
    halves = [[rcopy(f'h{a}{t}', src.at[pl.ds(t * sl + give, half), :], dst.at[t], peer) for t in range(N_TASK)]
              for a, (src, dst) in enumerate(((g1, rx1), (g2, rx2)))]
    for cp in halves[0] + halves[1]:
        cp.start()
    pairs = [(i, j) for i in range(N_TASK) for j in range(i, N_TASK)]
    acc = tuple(jnp.zeros((8, 128), F32) for _ in pairs)
    for a, (src, dst) in enumerate(((g1, rx1), (g2, rx2))):
        for cp in halves[a]:
            cp.wait_recv()

        def fold(r, acc):
            row = pl.multiple_of(r * 8, 8)
            acc = list(acc)
            for l in range(0, dim, 128):
                gs = []
                for t in range(N_TASK):
                    v = dst[t, pl.ds(row, 8), l:l + 128] + src[pl.ds(pl.multiple_of(t * sl + keep + row, 8), 8), l:l + 128]
                    dst[t, pl.ds(row, 8), l:l + 128] = v
                    gs.append(v)
                for q, (i, j) in enumerate(pairs):
                    acc[q] = acc[q] + gs[i] * gs[j]
            return tuple(acc)

        acc = lax.fori_loop(0, half // 8, fold, acc)
    gr_own[...] = jnp.zeros_like(gr_own)
    for q in range(len(pairs)):
        gr_own[q:q + 1, :] = jnp.sum(acc[q], axis=0, keepdims=True)
    loc = pltpu.make_async_copy(gr_own, gr_all.at[me], lsem.at[6])
    loc.start()
    grams = []
    for k in range(1, N_DEV):
        p = lax.rem(me + k, N_DEV)
        grams.append(rcopy(f'gram{k}', gr_own, gr_all.at[me], (p // N_DATA, lax.rem(p, N_DATA))))
        grams[-1].start()

    w_sends = list(wt.values()) + list(w_own.values()) + list(w_peer.values()) + list(w_fwd.values())
    for cp in (w_sends + first_x + first_y + more_x + more_y + [fwd_x, fwd_y] + z_x + z_y + z_d + e_twin + e_rest
               + halves[0] + halves[1]):
        cp.wait_send()

    for cp in grams:
        cp.wait()
    loc.wait()
    tot = gr_all[0]
    for k in range(1, N_DEV):
        tot = tot + gr_all[k]
    sums = jnp.broadcast_to(jnp.sum(tot, axis=1, keepdims=True), tot.shape)
    gram = {}
    for q, (i, j) in enumerate(pairs):
        gram[i, j] = gram[j, i] = sums[q:q + 1, :]
    scale = (gram[0, 0] + gram[1, 1] + gram[2, 2] + gram[3, 3]) / N_TASK

    def eg_step(k, w):
        up = []
        for i in range(N_TASK):
            mv = (gram[i, 0] * w[0] + gram[i, 1] * w[1]) + (gram[i, 2] * w[2] + gram[i, 3] * w[3])
            up.append(w[i] * jnp.exp(-mv / scale))
        s = (up[0] + up[1]) + (up[2] + up[3])
        return tuple(u / s for u in up)

    w = lax.fori_loop(0, STEPS, eg_step, tuple(jnp.full((1, 128), 1.0 / N_TASK, F32) for _ in range(N_TASK)))
    wts_ref[...] = jnp.zeros_like(wts_ref)
    for t in range(N_TASK):
        wts_ref[t:t + 1, :] = w[t]
    wb = [jnp.broadcast_to(v, (half, 128)) for v in w]

    def blend(rx, l):
        v = wb[0] * rx[0, :, l:l + 128]
        for t in range(1, N_TASK):
            v = v + wb[t] * rx[t, :, l:l + 128]
        return v

    for l in range(0, dim, 128):
        tr_ref[l:l + 128, 0:half] = blend(rx1, l).T
    outs = []
    for k in range(1, N_DATA):
        p = lax.rem(d + k, N_DATA)
        outs.append(rcopy(f'out{k}', tr_ref.at[pl.ds(pl.multiple_of(p * p1, p1), p1), :], rx_g1.at[d], (m, p)))
        outs[-1].start()
    loc = pltpu.make_async_copy(tr_ref.at[pl.ds(pl.multiple_of(d * p1, p1), p1), :], rx_g1.at[d], lsem.at[7])
    loc.start()
    for l in range(0, dim, 128):
        out2_ref[:, l:l + 128] = blend(rx2, l)
    loc.wait()
    for cp in outs:
        cp.wait()
    for k in range(N_DATA):
        out1_ref[:, k * half:(k + 1) * half] = rx_g1[k, :, 0:half]
    assert len(table) <= ssem.shape[0]


def mega_call(n_total, tokens, w_up, w_down, task_heads, labels):
    n_loc, dim = tokens.shape
    wide = w_up.shape[1]
    sl = 2 * wide // N_DATA
    half = sl // 2
    per = dim // N_DATA
    n_half = n_loc // 2
    vm = pl.BlockSpec(memory_space=pltpu.VMEM)
    hbm = pl.BlockSpec(memory_space=pl.ANY)
    vmem = pltpu.VMEM
    return pl.pallas_call(
        functools.partial(mega_kernel, n_total),
        out_shape=[jax.ShapeDtypeStruct((8, 128), F32), jax.ShapeDtypeStruct((per, half * N_DATA), F32),
                   jax.ShapeDtypeStruct((half, dim), F32)],
        in_specs=[hbm, hbm, hbm, vm, vm],
        out_specs=[vm, vm, vm],
        scratch_shapes=[vmem((4 * n_loc // BLK, BLK, dim), BF16), vmem((4 * n_loc // BLK, 16, BLK), F32),
                        vmem((dim, wide), BF16), vmem((wide, dim), BF16), vmem((dim, wide), BF16), vmem((wide, dim), BF16),
                        vmem((sl, dim), BF16), vmem((sl, dim), BF16),
                        vmem((N_TASK * N_CLASS, dim, 128), F32), vmem((24, dim), F32),
                        vmem((2, n_half // 2, dim), F32), vmem((2, n_half // 2, wide), BF16),
                        vmem((N_TASK * sl, dim), F32), vmem((N_TASK * sl, dim), F32),
                        vmem((N_TASK, half, dim), F32), vmem((N_TASK, half, dim), F32),
                        vmem((dim, BLK), BF16), vmem((dim, BLK), BF16), vmem((sl, BLK), BF16), vmem((sl, BLK), BF16),
                        vmem((sl, BLK), BF16), vmem((sl, BLK), BF16), vmem((sl, BLK), F32), vmem((sl, BLK), F32),
                        vmem((16, 128), F32), vmem((N_DEV, 16, 128), F32), vmem((dim, 256), F32), vmem((N_DATA, per, 256), F32),
                        pltpu.SemaphoreType.DMA((88,)), pltpu.SemaphoreType.DMA((88,)), pltpu.SemaphoreType.DMA((8,))],
        compiler_params=pltpu.CompilerParams(vmem_limit_bytes=VMEM_LIMIT, collective_id=0, has_side_effects=True),
    )(tokens, w_up, w_down, task_heads, labels)


def solution(mesh):
    n_data = mesh.shape['data']

    def local_step(tokens, w_up, w_down, task_heads, labels):
        wts, grad_up, grad_down = mega_call(tokens.shape[0] * n_data, tokens, w_up, w_down, task_heads, labels)
        return wts[:N_TASK, 0], grad_up, grad_down

    return jax.shard_map(
        local_step, mesh=mesh,
        in_specs=(P('data', None), P(None, 'model'), P('model', None), P(None, None, None), P(None, 'data')),
        out_specs=(P(None), P('data', 'model'), P(('model', 'data'), None)),
        check_vma=False)
```

```python
import functools

import jax
import jax.numpy as jnp
from jax import lax
from jax.experimental import pallas as pl
from jax.experimental.pallas import tpu as pltpu
from jax.sharding import PartitionSpec as P

STEPS = 20
MESH = pl.DeviceIdType.MESH
F32 = jnp.float32
BF16 = jnp.bfloat16
C0 = 0.7978845608028654
C1 = 0.044715
N_DATA = 8
N_DEV = 16
N_TASK = 4
N_CLASS = 3
BLK = 512
VMEM_LIMIT = 63 * 1024 * 1024


def gelu_only(a):
    return a * (0.5 + 0.5 * jnp.tanh(a * (C0 + (C0 * C1) * (a * a))))


def gelu_both(a):
    a2 = a * a
    t = jnp.tanh(a * (C0 + (C0 * C1) * a2))
    h = 0.5 + 0.5 * t
    slope = h + (0.5 * a) * (1.0 - t * t) * (C0 + (3.0 * C0 * C1) * a2)
    return a * h, slope


def nt_dot(a, b):
    return lax.dot_general(a, b, (((1,), (1,)), ((), ())), preferred_element_type=F32)


def nn_dot(a, b):
    return jnp.dot(a, b, preferred_element_type=F32)


def xor_data(d, dr):
    core = lax.rem(d, 2)
    x = lax.rem(d // 2, 2)
    y = d // 4
    return (lax.rem(y + dr // 2, 2) * 2 + lax.rem(x + dr % 2, 2)) * 2 + core


def dz_part(e_ref, s, t, hb_ref, dz):
    dim, blk = dz.shape
    rows = 32
    es = [[e_ref[s, N_TASK * c + t:N_TASK * c + t + 1, lo:lo + 128] for lo in range(0, blk, 128)] for c in range(N_CLASS - 1)]
    for r0 in range(0, dim, rows):
        h = [hb_ref[(N_CLASS - 1) * t + c, r0:r0 + rows, :] for c in range(N_CLASS - 1)]
        for j in range(blk // 128):
            val = h[0] * es[0][j] + h[1] * es[1][j]
            dz[r0:r0 + rows, 128 * j:128 * j + 128] = val.astype(BF16)


def act_part(x, w1t_ref, ut, sl, lo):
    act, slope = gelu_both(nt_dot(w1t_ref[...], x))
    ut[:, lo:lo + x.shape[0]] = act.astype(BF16)
    sl[:, lo:lo + x.shape[0]] = slope


def mega_kernel(n_total, x_hbm, w1_hbm, w2_hbm, heads_ref, lab_ref, wts_ref, out1_ref, out2_ref,
                x_all, e_all, w1v, w2v, w1f, w2f, w1t, w2s, hb, part, act_far, g1, g2, rx1, rx2,
                dz00, dz01, dz10, dz11, da00, da01, da10, da11, ut0, ut1, ut2, sl0, sl1, sl2, gr_own, gr_all, tr_ref, rx_g1,
                ssem, rsem, lsem, osend, orecv):
    m = lax.axis_index('model')
    d = lax.axis_index('data')
    core = lax.rem(d, 2)
    chip = d // 2
    me = m * N_DATA + d
    dim = x_all.shape[1]
    wide = w1v.shape[1]
    sl = w1t.shape[0]
    half = sl // 2
    p1 = dim // N_DATA
    p2 = wide // N_DATA

    def slot(k, lo=0, n=BLK):
        return x_all.at[pl.ds(k * BLK + lo, n), :]

    lcopy = [pltpu.make_async_copy(x_hbm.at[pl.ds(pl.multiple_of((2 * m + k) * BLK, BLK), BLK), :], slot(k), lsem.at[k])
             for k in range(2)]
    lcopy += [pltpu.make_async_copy(w1_hbm, w1v, lsem.at[2]), pltpu.make_async_copy(w2_hbm, w2v, lsem.at[3])]
    lcopy += [pltpu.make_async_copy(x_hbm.at[pl.ds(pl.multiple_of((2 - 2 * m + k) * BLK, BLK), BLK), :], slot(2 + k),
                                    lsem.at[4 + k]) for k in range(2)]
    for cp in lcopy:
        cp.start()

    barrier = pltpu.get_barrier_semaphore()
    for k in range(1, N_DEV):
        p = lax.rem(me + k, N_DEV)
        pl.semaphore_signal(barrier, inc=1, device_id=(p // N_DATA, lax.rem(p, N_DATA)), device_id_type=MESH)
    pl.semaphore_wait(barrier, N_DEV - 1)

    twin = (1 - m, d)
    peer = (m, d + 1 - 2 * core)
    nb_x = (m, xor_data(d, 1))
    nb_y = (m, xor_data(d, 2))

    table = {}

    def rcopy(name, src, dst, dev):
        if name not in table:
            table[name] = len(table)
        k = table[name]
        return pltpu.make_async_remote_copy(src, dst, ssem.at[k], rsem.at[k], device_id=dev, device_id_type=MESH)

    def w1_rows(dr):
        return w1f.at[pl.ds(pl.multiple_of(xor_data(d, dr) * p1, p1), p1), :]

    def w2_rows(dr):
        return w2f.at[pl.ds(pl.multiple_of(xor_data(d, dr) * p2, p2), p2), :]

    rows_of = {1: w1_rows, 2: w2_rows}

    def w_copy(w, name, dr, dev):
        return rcopy(f'w{w}{name}', rows_of[w](dr), rows_of[w](dr), dev)

    wt = {1: rcopy('w1t', w1_hbm.at[pl.ds(pl.multiple_of(d * p1, p1), p1), :], w1_rows(0), twin),
          2: rcopy('w2t', w2_hbm.at[pl.ds(pl.multiple_of(d * p2, p2), p2), :], w2_rows(0), twin)}
    w_own = {(w, n): w_copy(w, 'own' + n, 0, dev) for w in (1, 2) for n, dev in (('p', peer), ('x', nb_x), ('y', nb_y))}
    w_peer = {(w, dr): w_copy(w, f'peer{dr}', dr, peer) for w in (1, 2) for dr in (1, 2, 3)}
    w_diag = {1: rcopy('w1d', w1_hbm.at[pl.ds(pl.multiple_of(xor_data(d, 3) * p1, p1), p1), :], w1_rows(3), twin),
              2: rcopy('w2d', w2_hbm.at[pl.ds(pl.multiple_of(xor_data(d, 3) * p2, p2), p2), :], w2_rows(3), twin)}

    def own_block(b, lo, n):
        return x_hbm.at[pl.ds(pl.multiple_of(b * BLK + lo, BLK // 2), n), :]

    hb2 = BLK // 2
    first_x = [rcopy(f'fx{h}', own_block(3 * m, h * hb2, hb2), slot(4, h * hb2, hb2), nb_x) for h in (0, 1)]
    first_y = [rcopy(f'fy{h}', own_block(1 + m, h * hb2, hb2), slot(5, h * hb2, hb2), nb_y) for h in (0, 1)]
    more_x = [rcopy(f'mx{b}', own_block(b, 0, BLK), slot(k), nb_x) for b, k in ((1, 10), (2, 13))]
    more_y = [rcopy(f'my{b}', own_block(b, 0, BLK), slot(k), nb_y) for b, k in ((0, 11), (3, 14))]
    fwd_x = [rcopy(f'dx{h}', slot(5, h * hb2, hb2), slot(6, h * hb2, hb2), nb_x) for h in (0, 1)]
    fwd_y = [rcopy(f'dy{h}', slot(4, h * hb2, hb2), slot(7, h * hb2, hb2), nb_y) for h in (0, 1)]
    z_x = [rcopy(f'zx{h}', slot(4, h * hb2, hb2), slot(8, h * hb2, hb2), twin) for h in (0, 1)]
    z_y = [rcopy(f'zy{h}', slot(5, h * hb2, hb2), slot(9, h * hb2, hb2), twin) for h in (0, 1)]
    z_d = [rcopy('zd6', slot(6), slot(12), twin), rcopy('zd7', slot(7), slot(15), twin)]

    k_out, k_in = m, 1 - m
    e_twin = [rcopy(f'et{k}', e_all.at[k], e_all.at[2 + k], twin) for k in range(2)]
    e_rest = []
    for dz in (0, 1):
        for dr in (1, 2, 3):
            dev = (lax.rem(m + dz, 2), xor_data(d, dr))
            s_out, s_in = {1: (4 + 4 * dz, 10 + 3 * m), 2: (11 + 3 * m, 5 + 4 * dz), 3: (7 + 8 * dz, 6 + 6 * dz)}[dr]
            e_rest.append(rcopy(f'eo{dz}{dr}', e_all.at[k_out], e_all.at[s_out], dev))
            e_rest.append(rcopy(f'ei{dz}{dr}', e_all.at[k_in], e_all.at[s_in], dev))

    wt[1].start()
    first_x[0].start()
    first_y[0].start()
    wt[2].start()
    w_diag[1].start()
    w_diag[2].start()

    for c in range(N_CLASS - 1):
        h = heads_ref[c].astype(F32) - heads_ref[N_CLASS - 1].astype(F32)
        h = jnp.concatenate([h, h], axis=0).T
        for t in range(N_TASK):
            hb[(N_CLASS - 1) * t + c] = jnp.broadcast_to(h[:, t:t + 1], (dim, 128))
    for k in range(4):
        lcopy[k].wait()
    off = pl.multiple_of(chip * sl, sl)
    w1t[...] = w1v[:, pl.ds(off, sl)].T
    w2s[...] = w2v[pl.ds(off, sl), :]

    fc = wide // 3

    def part_block(k):
        x = x_all[k * BLK:(k + 1) * BLK, :]
        acc = None
        for f in range(0, wide, fc):
            u = gelu_only(nn_dot(x, w1v[:, f:f + fc])).astype(BF16)
            y = nn_dot(u, w2v[f:f + fc, :])
            acc = y if acc is None else acc + y
        part[k] = acc

    with jax.named_scope('near'):
        part_block(0)
        wt[1].wait_recv()
        for n in 'xyp':
            w_own[1, n].start()
        part_block(1)
        wt[2].wait_recv()
        for n in 'xyp':
            w_own[2, n].start()
        first_x[1].start()
        first_y[1].start()
        first_x[0].wait_recv()
        z_x[0].start()
        first_y[0].wait_recv()
        fwd_x[0].start()
        fwd_y[0].start()
        act_part(x_all[0:BLK, :], w1t, ut0, sl0, 0)
        g1[...] = jnp.zeros_like(g1)
        g2[...] = jnp.zeros_like(g2)
    with jax.named_scope('wait_w1'):
        w_own[1, 'x'].wait_recv()
        w_peer[1, 1].start()
        w_own[1, 'y'].wait_recv()
        w_peer[1, 2].start()
        w_diag[1].wait_recv()
        w_peer[1, 3].start()
        w_own[1, 'p'].wait_recv()
        for dr in (1, 2, 3):
            w_peer[1, dr].wait_recv()
    with jax.named_scope('far1'):
        for k in range(2):
            x = x_all[k * BLK:(k + 1) * BLK, :]
            for f in range(0, wide, fc):
                act_far[k, :, f:f + fc] = gelu_only(nn_dot(x, w1f[:, f:f + fc])).astype(BF16)
    def w2_chunk(k, dr):
        rows = pl.ds(pl.multiple_of((xor_data(d, dr) // 2) * sl, sl), sl)
        part[k] += nn_dot(act_far[k, :, rows], w2f[rows, :])

    with jax.named_scope('wait_w2'):
        w_own[2, 'x'].wait_recv()
        w_peer[2, 1].start()
        w_own[2, 'y'].wait_recv()
        w_peer[2, 2].start()
        w_own[2, 'p'].wait_recv()
        for k in range(2):
            w2_chunk(k, 0)
        for dr in (1, 2):
            w_peer[2, dr].wait_recv()
            for k in range(2):
                w2_chunk(k, dr)
        w_diag[2].wait_recv()
        w_peer[2, 3].start()
        w_peer[2, 3].wait_recv()
    with jax.named_scope('errs'):
        heads16 = jnp.concatenate([heads_ref[c] for c in range(N_CLASS)] + [heads_ref[0]], axis=0)
        for k in range(2):
            w2_chunk(k, 3)
            z = (x_all[k * BLK:(k + 1) * BLK, :].astype(F32) + part[k]).astype(BF16)
            logits = nt_dot(heads16, z)
            lg = [logits[N_TASK * c:N_TASK * c + N_TASK, :] for c in range(N_CLASS)]
            top = jnp.maximum(jnp.maximum(lg[0], lg[1]), lg[2])
            ex = [jnp.exp(v - top) for v in lg]
            tot = ex[0] + ex[1] + ex[2]
            lab = lab_ref[:, pl.ds(pl.multiple_of((2 * m + k) * BLK, BLK), BLK)]
            for c in range(N_CLASS - 1):
                rest = (ex[1 - c] + ex[2]) / tot
                e_all[k, N_TASK * c:N_TASK * c + N_TASK, :] = jnp.where(lab == c, -rest, ex[c] / tot) * (1.0 / n_total)
        for cp in e_twin + e_rest:
            cp.start()
        z_y[0].start()

    dzs, das, uts, sls = ((dz00, dz01), (dz10, dz11)), ((da00, da01), (da10, da11)), (ut0, ut1, ut2), (sl0, sl1, sl2)
    n_blk = x_all.shape[0] // BLK
    keep_row = pl.multiple_of(core * half, half)
    give_row = pl.multiple_of((1 - core) * half, half)
    keep_col = pl.multiple_of(core * (dim // 2), 128)
    give_col = pl.multiple_of((1 - core) * (dim // 2), 128)
    halves = [(rcopy(f'h1{t}', g1.at[pl.ds(t * sl, sl), pl.ds(give_col, dim // 2)], rx1.at[t], peer),
               rcopy(f'h2{t}', g2.at[pl.ds(t * sl + give_row, half), :], rx2.at[t], peer)) for t in range(N_TASK)]

    with jax.named_scope('lead_in'):
        dz_part(e_all, 0, 0, hb, dz00)
        first_x[1].wait_recv()
        first_y[1].wait_recv()
        for cp in (fwd_x[1], fwd_y[1], z_x[1], z_y[1], more_x[0], more_y[0], more_x[1], more_y[1]):
            cp.start()

    def links_2():
        for cp in fwd_x + fwd_y:
            cp.wait_recv()
        for cp in z_d:
            cp.start()

    def arrive(*cps):
        def go():
            for cp in cps:
                cp.wait_recv()
        return go

    lcopy[4].wait()
    lcopy[5].wait()
    actions = {1: arrive(*e_twin), 3: arrive(*e_rest), 5: links_2, 7: arrive(*z_x), 8: arrive(*z_y), 9: arrive(more_x[0]),
               10: arrive(more_y[0]), 11: arrive(z_d[0]), 12: arrive(more_x[1]), 13: arrive(more_y[1])}

    def tok(b, lo=0, n=BLK):
        return pl.ds(pl.multiple_of(b * BLK + lo, 256), n)

    def total(parts):
        out = parts[0]
        for v in parts[1:]:
            out = out + v
        return out

    def group(blks, nxt, last):
        hw = BLK // 2
        for t in range(N_TASK):
            dz, da = dzs[t % 2], das[t % 2]
            rows = slice(t * sl, (t + 1) * sl)
            for b, u, h in blks:
                da[h][...] = (nn_dot(w2s[...], dz[h][...]) * sls[u][...]).astype(BF16)
            if t < N_TASK - 1:
                for b, u, h in blks:
                    dz_part(e_all, b, t + 1, hb, dzs[(t + 1) % 2][h])
            elif nxt is not None:
                dz_part(e_all, nxt[0], 0, hb, dzs[0][nxt[2]])
            if t < 2 and nxt is not None:
                act_part(x_all[tok(nxt[0], t * hw, hw), :], w1t, uts[nxt[1]], sls[nxt[1]], t * hw)
            g2[rows, :] += total([nt_dot(uts[u][...], dz[h][...]) for b, u, h in blks])
            g1[rows, :] += total([nn_dot(da[h][...], x_all[tok(b), :]) for b, u, h in blks])
            if last:
                for cp in halves[t]:
                    cp.start()

    def body(i, c):
        for q in (0, 1):
            for k, act in actions.items():
                if k % 2 == q:
                    @pl.when(i == k // 2)
                    def _():
                        with jax.named_scope(f'arr{k}'):
                            act()
            group([(2 * i + q, q, 0)], (2 * i + q + 1, 1 - q, 0), False)
        return c

    with jax.named_scope('main'):
        lax.fori_loop(0, n_blk // 2 - 1, body, 0)
    with jax.named_scope('last_act'):
        z_d[1].wait_recv()
        act_part(x_all[tok(n_blk - 1), :], w1t, ut2, sl2, 0)
        dz_part(e_all, n_blk - 1, 0, hb, dz01)
    with jax.named_scope('main_last'):
        group([(n_blk - 2, 0, 0), (n_blk - 1, 2, 1)], None, True)

    with jax.named_scope('halves'):
        pairs = [(i, j) for i in range(N_TASK) for j in range(i, N_TASK)]
        acc = tuple(jnp.zeros((8, 128), F32) for _ in pairs)

        def fold(new, old, acc):
            def one(src, dst, n_rows, n_cols, row_of, col0, acc):
                def go(r, acc):
                    row = pl.multiple_of(r * 8, 8)
                    acc = list(acc)
                    for l in range(0, n_cols, 128):
                        gs = {t: dst[t, pl.ds(row, 8), l:l + 128] for t in old}
                        for t in new:
                            v = dst[t, pl.ds(row, 8), l:l + 128] + src[pl.ds(pl.multiple_of(row_of(t) + row, 8), 8),
                                                                       pl.ds(pl.multiple_of(col0 + l, 128), 128)]
                            dst[t, pl.ds(row, 8), l:l + 128] = v
                            gs[t] = v
                        for q, (i, j) in enumerate(pairs):
                            if (i in new or j in new) and i in gs and j in gs:
                                acc[q] = acc[q] + gs[i] * gs[j]
                    return tuple(acc)
                return lax.fori_loop(0, n_rows // 8, go, acc)

            for t in new:
                for cp in halves[t]:
                    cp.wait_recv()
            acc = one(g1, rx1, sl, dim // 2, lambda t: t * sl, keep_col, acc)
            return one(g2, rx2, half, dim, lambda t: t * sl + keep_row, 0, acc)

        acc = fold((0, 1, 2), (), acc)
        acc = fold((3,), (0, 1, 2), acc)
    with jax.named_scope('gram_x'):
        gr_own[...] = jnp.zeros_like(gr_own)
        for q in range(len(pairs)):
            gr_own[q:q + 1, :] = jnp.sum(acc[q], axis=0, keepdims=True)
        loc = pltpu.make_async_copy(gr_own, gr_all.at[me], lsem.at[6])
        loc.start()
        grams = []
        for k in range(1, N_DEV):
            p = lax.rem(me + k, N_DEV)
            grams.append(rcopy(f'gram{k}', gr_own, gr_all.at[me], (p // N_DATA, lax.rem(p, N_DATA))))
            grams[-1].start()

        w_sends = list(wt.values()) + list(w_own.values()) + list(w_peer.values()) + list(w_diag.values())
        for cp in (w_sends + first_x + first_y + more_x + more_y + fwd_x + fwd_y + z_x + z_y + z_d + e_twin + e_rest
                   + [cp for h in halves for cp in h]):
            cp.wait_send()

        for cp in grams:
            cp.wait()
        loc.wait()
    with jax.named_scope('weights'):
        tot = gr_all[0]
        for k in range(1, N_DEV):
            tot = tot + gr_all[k]
        sums = jnp.broadcast_to(jnp.sum(tot, axis=1, keepdims=True), tot.shape)
        gram = {}
        for q, (i, j) in enumerate(pairs):
            gram[i, j] = gram[j, i] = sums[q:q + 1, :]
        scale = (gram[0, 0] + gram[1, 1] + gram[2, 2] + gram[3, 3]) / N_TASK

        def eg_step(k, w):
            up = []
            for i in range(N_TASK):
                mv = (gram[i, 0] * w[0] + gram[i, 1] * w[1]) + (gram[i, 2] * w[2] + gram[i, 3] * w[3])
                up.append(w[i] * jnp.exp(-mv / scale))
            s = (up[0] + up[1]) + (up[2] + up[3])
            return tuple(u / s for u in up)

        w = lax.fori_loop(0, STEPS, eg_step, tuple(jnp.full((1, 128), 1.0 / N_TASK, F32) for _ in range(N_TASK)))
        wts_ref[...] = jnp.zeros_like(wts_ref)
        for t in range(N_TASK):
            wts_ref[t:t + 1, :] = w[t]
    def blend(rx, l):
        wb = [jnp.broadcast_to(v, (rx.shape[1], 128)) for v in w]
        v = wb[0] * rx[0, :, l:l + 128]
        for t in range(1, N_TASK):
            v = v + wb[t] * rx[t, :, l:l + 128]
        return v

    with jax.named_scope('outs'):
        cols = pl.ds(pl.multiple_of(chip * sl, sl), sl)
        n_dest = N_DATA // 2
        outs = []
        for j in range(n_dest):
            p = n_dest * core + j
            src = tr_ref.at[j * p1:(j + 1) * p1, :]
            outs.append((p, pltpu.make_async_remote_copy(src, rx_g1.at[:, cols], osend.at[j], orecv.at[chip],
                                                         device_id=(m, p), device_id_type=MESH),
                         pltpu.make_async_copy(src, rx_g1.at[:, cols], lsem.at[7])))
        for l in range(0, dim // 2, 128):
            tr_ref[l:l + 128, :] = blend(rx1, l).T
        for p, far, near in outs:
            @pl.when(p != d)
            def _():
                far.start()

            @pl.when(p == d)
            def _():
                near.start()
        for l in range(0, dim, 128):
            out2_ref[:, l:l + 128] = blend(rx2, l)
        for k in range(N_DATA // 2):
            @pl.when(jnp.logical_or(core != d // n_dest, chip != k))
            def _():
                pltpu.make_async_remote_copy(tr_ref.at[0:p1, :], rx_g1.at[:, k * sl:(k + 1) * sl], osend.at[0], orecv.at[k],
                                             device_id=peer, device_id_type=MESH).wait_recv()
        for p, far, near in outs:
            @pl.when(p != d)
            def _():
                far.wait_send()

            @pl.when(p == d)
            def _():
                near.wait()
        out1_ref[...] = rx_g1[...]
    assert len(table) <= ssem.shape[0]


def mega_call(n_total, tokens, w_up, w_down, task_heads, labels):
    n_loc, dim = tokens.shape
    wide = w_up.shape[1]
    sl = 2 * wide // N_DATA
    half = sl // 2
    per = dim // N_DATA
    n_half = n_loc // 2
    vm = pl.BlockSpec(memory_space=pltpu.VMEM)
    hbm = pl.BlockSpec(memory_space=pl.ANY)
    vmem = pltpu.VMEM
    return pl.pallas_call(
        functools.partial(mega_kernel, n_total),
        out_shape=[jax.ShapeDtypeStruct((8, 128), F32), jax.ShapeDtypeStruct((per, half * N_DATA), F32),
                   jax.ShapeDtypeStruct((half, dim), F32)],
        in_specs=[hbm, hbm, hbm, vm, vm],
        out_specs=[vm, vm, vm],
        scratch_shapes=[vmem((4 * n_loc, dim), BF16), vmem((4 * n_loc // BLK, 8, BLK), F32),
                        vmem((dim, wide), BF16), vmem((wide, dim), BF16), vmem((dim, wide), BF16), vmem((wide, dim), BF16),
                        vmem((sl, dim), BF16), vmem((sl, dim), BF16),
                        vmem((N_TASK * (N_CLASS - 1), dim, 128), F32),
                        vmem((2, n_half // 2, dim), F32), vmem((2, n_half // 2, wide), BF16),
                        vmem((N_TASK * sl, dim), F32), vmem((N_TASK * sl, dim), F32),
                        vmem((N_TASK, sl, dim // 2), F32), vmem((N_TASK, half, dim), F32),
                        *[vmem((dim, BLK), BF16)] * 4, *[vmem((sl, BLK), BF16)] * 7, *[vmem((sl, BLK), F32)] * 3,
                        vmem((16, 128), F32), vmem((N_DEV, 16, 128), F32), vmem((dim // 2, sl), F32), vmem((per, wide), F32),
                        pltpu.SemaphoreType.DMA((88,)), pltpu.SemaphoreType.DMA((88,)), pltpu.SemaphoreType.DMA((8,)),
                        pltpu.SemaphoreType.DMA((4,)), pltpu.SemaphoreType.DMA((4,))],
        compiler_params=pltpu.CompilerParams(vmem_limit_bytes=VMEM_LIMIT, collective_id=0, has_side_effects=True),
    )(tokens, w_up, w_down, task_heads, labels)


def final_kernel(wts_in, g1_in, g2_in, wts_ref, g1_ref, g2_ref):
    for t in range(N_TASK):
        wts_ref[t] = wts_in[t, 0]
    g1_ref[...] = g1_in[...]
    g2_ref[...] = g2_in[...]


def final_call(wts, g1, g2):
    vm = pl.BlockSpec(memory_space=pltpu.VMEM)
    return pl.pallas_call(
        final_kernel,
        out_shape=[jax.ShapeDtypeStruct((N_TASK,), F32), jax.ShapeDtypeStruct(g1.shape, F32), jax.ShapeDtypeStruct(g2.shape, F32)],
        in_specs=[vm, vm, vm],
        out_specs=[pl.BlockSpec(memory_space=pltpu.SMEM), vm, vm],
        compiler_params=pltpu.CompilerParams(vmem_limit_bytes=VMEM_LIMIT),
    )(wts, g1, g2)


def solution(mesh):
    n_data = mesh.shape['data']

    def local_step(tokens, w_up, w_down, task_heads, labels):
        wts, up, down = mega_call(tokens.shape[0] * n_data, tokens, w_up, w_down, task_heads.transpose(2, 0, 1), labels)
        return final_call(wts, up, down)

    return jax.shard_map(
        local_step, mesh=mesh,
        in_specs=(P('data', None), P(None, 'model'), P('model', None), P(None, None, None), P(None, 'data')),
        out_specs=(P(None), P('data', 'model'), P(('model', 'data'), None)),
        check_vma=False)
```

```python
import functools

import jax
import jax.numpy as jnp
from jax import lax
from jax.experimental import pallas as pl
from jax.experimental.pallas import tpu as pltpu
from jax.sharding import PartitionSpec as P

STEPS = 20
MESH = pl.DeviceIdType.MESH
F32 = jnp.float32
BF16 = jnp.bfloat16
C0 = 0.7978845608028654
C1 = 0.044715
N_DATA = 8
N_DEV = 16
N_TASK = 4
N_CLASS = 3
BLK = 512
VMEM_LIMIT = 63 * 1024 * 1024


def gelu_only(a):
    return a * (0.5 + 0.5 * jnp.tanh(a * (C0 + (C0 * C1) * (a * a))))


def gelu_both(a):
    a2 = a * a
    t = jnp.tanh(a * (C0 + (C0 * C1) * a2))
    h = 0.5 + 0.5 * t
    act = a * h
    return act, h + act * (1.0 - h) * (2.0 * C0 + (6.0 * C0 * C1) * a2)


def nt_dot(a, b):
    return lax.dot_general(a, b, (((1,), (1,)), ((), ())), preferred_element_type=F32)


def nn_dot(a, b):
    return jnp.dot(a, b, preferred_element_type=F32)


def xor_data(d, dr):
    core = lax.rem(d, 2)
    x = lax.rem(d // 2, 2)
    y = d // 4
    return (lax.rem(y + dr // 2, 2) * 2 + lax.rem(x + dr % 2, 2)) * 2 + core


def dz_part(e_ref, s, t, hb_ref, dz):
    dim, blk = dz.shape
    rows = 32
    es = [[e_ref[s, N_TASK * c + t:N_TASK * c + t + 1, lo:lo + 128] for lo in range(0, blk, 128)] for c in range(N_CLASS - 1)]
    for r0 in range(0, dim, rows):
        h = [hb_ref[(N_CLASS - 1) * t + c, r0:r0 + rows, :] for c in range(N_CLASS - 1)]
        for j in range(blk // 128):
            val = h[0] * es[0][j] + h[1] * es[1][j]
            dz[r0:r0 + rows, 128 * j:128 * j + 128] = val.astype(BF16)


def act_part(x, w1t_ref, ut, sl):
    act, slope = gelu_both(nt_dot(w1t_ref[...], x))
    ut[...] = act.astype(BF16)
    sl[...] = slope


def mega_kernel(n_total, x_hbm, w1_hbm, w2_hbm, heads_ref, lab_ref, wts_ref, out1_ref, out2_ref,
                x_all, e_all, w1v, w2v, w1f, w2f, w1t, w2s, hb, part, act_far, g1, g2, rx1, rx2,
                dz00, dz01, dz10, dz11, da00, da01, da10, da11, ut_own, sl_own, gr_own, gr_all, tr_ref, rx_g1,
                ssem, rsem, lsem, osend, orecv):
    m = lax.axis_index('model')
    d = lax.axis_index('data')
    core = lax.rem(d, 2)
    chip = d // 2
    me = m * N_DATA + d
    dim = x_all.shape[1]
    wide = w1v.shape[1]
    sl = w1t.shape[0]
    half = sl // 2
    p1 = dim // N_DATA
    p2 = wide // N_DATA

    def slot(k, lo=0, n=BLK):
        return x_all.at[pl.ds(k * BLK + lo, n), :]

    lcopy = [pltpu.make_async_copy(x_hbm.at[pl.ds(pl.multiple_of((2 * m + k) * BLK, BLK), BLK), :], slot(k), lsem.at[k])
             for k in range(2)]
    lcopy += [pltpu.make_async_copy(w1_hbm, w1v, lsem.at[2]), pltpu.make_async_copy(w2_hbm, w2v, lsem.at[3])]
    lcopy += [pltpu.make_async_copy(x_hbm.at[pl.ds(pl.multiple_of((2 - 2 * m + k) * BLK, BLK), BLK), :], slot(2 + k),
                                    lsem.at[4 + k]) for k in range(2)]
    for cp in lcopy:
        cp.start()

    barrier = pltpu.get_barrier_semaphore()
    for k in range(1, N_DEV):
        p = lax.rem(me + k, N_DEV)
        pl.semaphore_signal(barrier, inc=1, device_id=(p // N_DATA, lax.rem(p, N_DATA)), device_id_type=MESH)
    pl.semaphore_wait(barrier, N_DEV - 1)

    twin = (1 - m, d)
    peer = (m, d + 1 - 2 * core)
    nb_x = (m, xor_data(d, 1))
    nb_y = (m, xor_data(d, 2))

    table = {}

    def rcopy(name, src, dst, dev):
        if name not in table:
            table[name] = len(table)
        k = table[name]
        return pltpu.make_async_remote_copy(src, dst, ssem.at[k], rsem.at[k], device_id=dev, device_id_type=MESH)

    def w_rows(w, dr, part=None, ref=None):
        n = p1 if w == 1 else p2
        lo, size = (0, n) if part is None else (part * (n // 2), n // 2)
        ref = (w1f if w == 1 else w2f) if ref is None else ref
        return ref.at[pl.ds(pl.multiple_of(xor_data(d, dr) * n + lo, n // 2), size), :]

    w_hbm = {1: w1_hbm, 2: w2_hbm}
    wt = {(w, h): rcopy(f't{w}{h}', w_rows(w, 0, h, w_hbm[w]), w_rows(w, 0, h), twin) for w in (1, 2) for h in (0, 1)}
    wd = {1: rcopy('d1', w_rows(1, 3, 1, w1_hbm), w_rows(1, 3, 1), twin), 2: rcopy('d2', w_rows(2, 3, None, w2_hbm), w_rows(2, 3), twin)}
    w_own = {(w, h, n): rcopy(f'o{w}{h}{n}', w_rows(w, 0, h), w_rows(w, 0, h), dev)
             for w in (1, 2) for h in (0, 1) for n, dev in (('x', nb_x), ('y', nb_y))}
    w_peer = {(w, dr): rcopy(f'p{w}{dr}', w_rows(w, dr), w_rows(w, dr), peer) for w in (1, 2) for dr in range(4)}
    w_fwd = rcopy('g0', w_rows(1, 1, 0), w_rows(1, 1, 0), nb_y)

    pieces = ((0, BLK // 4), (BLK // 4, BLK // 4), (BLK // 2, BLK // 2))

    def own_piece(b, lo, n):
        return x_hbm.at[pl.ds(pl.multiple_of(b * BLK + lo, BLK // 4), n), :]

    def cut(name, src, dst, dev):
        return [rcopy(f'{name}{lo}', slot(src, lo, n), slot(dst, lo, n), dev) for lo, n in pieces]

    first_x = [rcopy(f'fx{lo}', own_piece(3 * m, lo, n), slot(4, lo, n), nb_x) for lo, n in pieces]
    first_y = [rcopy(f'fy{lo}', own_piece(1 + m, lo, n), slot(5, lo, n), nb_y) for lo, n in pieces]
    more_x = [rcopy(f'mx{b}', own_piece(b, 0, BLK), slot(k), nb_x) for b, k in ((1, 10), (2, 13))]
    more_y = [rcopy(f'my{k}', own_piece(b, 0, BLK), slot(k), nb_y) for b, k in ((3 - 3 * m, 11), (3 * m, 14))]
    fwd_x = cut('dx', 5, 7, nb_x)
    fwd_y = cut('dy', 4, 8, nb_y)
    z_x = cut('zx', 4, 6, twin)
    z_y = cut('zy', 5, 9, twin)
    keep15 = BLK - BLK // 4
    z_d = [rcopy('zd7', slot(7), slot(12), twin), rcopy('zd8', slot(8, 0, keep15), slot(15, 0, keep15), twin)]
    last_x = rcopy('lx', slot(11, keep15, BLK // 4), slot(15, keep15, BLK // 4), nb_x)

    k_out, k_in = m, 1 - m
    e_twin = [rcopy(f'et{k}', e_all.at[k], e_all.at[2 + k], twin) for k in range(2)]
    e_rest = []
    for dz in (0, 1):
        for dr in (1, 2, 3):
            dev = (lax.rem(m + dz, 2), xor_data(d, dr))
            s_out, s_in = {1: (4 + 2 * dz, 10 + 3 * m), 2: (14 - 3 * dz, 5 + 4 * dz), 3: (8 + 7 * dz, 7 + 5 * dz)}[dr]
            e_rest.append(rcopy(f'eo{dz}{dr}', e_all.at[k_out], e_all.at[s_out], dev))
            e_rest.append(rcopy(f'ei{dz}{dr}', e_all.at[k_in], e_all.at[s_in], dev))

    wt[1, 0].start()
    wt[1, 1].start()
    first_x[0].start()
    first_y[0].start()
    wt[2, 0].start()
    wt[2, 1].start()
    wd[1].start()
    wd[2].start()
    for k in range(4):
        lcopy[k].wait()

    fc = wide // 3

    def part_block(k):
        x = x_all[k * BLK:(k + 1) * BLK, :]
        acc = None
        for f in range(0, wide, fc):
            u = gelu_only(nn_dot(x, w1v[:, f:f + fc])).astype(BF16)
            y = nn_dot(u, w2v[f:f + fc, :])
            acc = y if acc is None else acc + y
        part[k] = acc

    def act_own(k):
        act_part(x_all[k * BLK:(k + 1) * BLK, :], w1t, ut_own.at[k], sl_own.at[k])

    with jax.named_scope('near'):
        part_block(0)
        wt[1, 0].wait_recv()
        for n in 'xy':
            w_own[1, 0, n].start()
        for c in range(N_CLASS - 1):
            h = heads_ref[c].astype(F32) - heads_ref[N_CLASS - 1].astype(F32)
            h = jnp.concatenate([h, h], axis=0).T
            for t in range(N_TASK):
                hb[(N_CLASS - 1) * t + c] = jnp.broadcast_to(h[:, t:t + 1], (dim, 128))
        off = pl.multiple_of(chip * sl, sl)
        w1t[...] = w1v[:, pl.ds(off, sl)].T
        w2s[...] = w2v[pl.ds(off, sl), :]
        wt[1, 1].wait_recv()
        for n in 'xy':
            w_own[1, 1, n].start()
        w_peer[1, 0].start()
        part_block(1)
    with jax.named_scope('wait_t2'):
        w_own[1, 0, 'x'].wait_recv()
        w_fwd.start()
        wt[2, 0].wait_recv()
        for n in 'xy':
            w_own[2, 0, n].start()
        for n, dr, hs in (('x', 1, (1,)), ('y', 2, (0, 1))):
            for h in hs:
                w_own[1, h, n].wait_recv()
            w_peer[1, dr].start()
        wt[2, 1].wait_recv()
        for n in 'xy':
            w_own[2, 1, n].start()
        w_peer[2, 0].start()
        for j in (1, 2):
            first_x[j].start()
            first_y[j].start()
    for k in (4, 5):
        lcopy[k].wait()
    act_own(0)
    act_own(1)
    first_x[0].wait_recv()
    z_x[0].start()
    first_y[0].wait_recv()
    act_own(2)
    act_own(3)
    with jax.named_scope('wait_w1'):
        w_fwd.wait_recv()
        wd[1].wait_recv()
        w_peer[1, 3].start()
        for h in (0, 1):
            w_own[2, h, 'x'].wait_recv()
        w_peer[2, 1].start()
        for dr in range(4):
            w_peer[1, dr].wait_recv()
    with jax.named_scope('far1'):
        for k in range(2):
            x = x_all[k * BLK:(k + 1) * BLK, :]
            for f in range(0, wide, fc):
                act_far[k, :, f:f + fc] = gelu_only(nn_dot(x, w1f[:, f:f + fc])).astype(BF16)
    def w2_pair(k, j):
        rows = pl.ds(pl.multiple_of(lax.rem(chip // 2 + j, 2) * (2 * sl), 2 * sl), 2 * sl)
        part[k] += nn_dot(act_far[k, :, rows], w2f[rows, :])

    with jax.named_scope('wait_w2'):
        for h in (0, 1):
            w_own[2, h, 'y'].wait_recv()
        w_peer[2, 2].start()
        for dr in (0, 1):
            w_peer[2, dr].wait_recv()
        w2_pair(0, 0)
        wd[2].wait_recv()
        w_peer[2, 3].start()
        g1[...] = jnp.zeros_like(g1)
        g2[...] = jnp.zeros_like(g2)
        w2_pair(1, 0)
        for dr in (2, 3):
            w_peer[2, dr].wait_recv()
    with jax.named_scope('errs'):
        heads16 = jnp.concatenate([heads_ref[c] for c in range(N_CLASS)] + [heads_ref[0]], axis=0)
        for k in range(2):
            w2_pair(k, 1)
            z = (x_all[k * BLK:(k + 1) * BLK, :].astype(F32) + part[k]).astype(BF16)
            logits = nt_dot(heads16, z)
            lg = [logits[N_TASK * c:N_TASK * c + N_TASK, :] for c in range(N_CLASS)]
            top = jnp.maximum(jnp.maximum(lg[0], lg[1]), lg[2])
            ex = [jnp.exp(v - top) for v in lg]
            tot = ex[0] + ex[1] + ex[2]
            lab = lab_ref[:, pl.ds(pl.multiple_of((2 * m + k) * BLK, BLK), BLK)]
            for c in range(N_CLASS - 1):
                rest = (ex[1 - c] + ex[2]) / tot
                e_all[k, N_TASK * c:N_TASK * c + N_TASK, :] = jnp.where(lab == c, -rest, ex[c] / tot) * (1.0 / n_total)
        for cp in e_twin + e_rest:
            cp.start()
        for cp in (z_y[0], fwd_x[0], fwd_y[0]):
            cp.start()

    dzs, das = ((dz00, dz01), (dz10, dz11)), ((da00, da01), (da10, da11))
    n_blk = x_all.shape[0] // BLK
    keep_row = pl.multiple_of(core * half, half)
    give_row = pl.multiple_of((1 - core) * half, half)
    keep_col = pl.multiple_of(core * (dim // 2), 128)
    give_col = pl.multiple_of((1 - core) * (dim // 2), 128)
    halves = [(rcopy(f'h1{t}', g1.at[pl.ds(t * sl, sl), pl.ds(give_col, dim // 2)], rx1.at[t], peer),
               rcopy(f'h2{t}', g2.at[pl.ds(t * sl + give_row, half), :], rx2.at[t], peer)) for t in range(N_TASK)]

    def relay(j):
        for cp in (first_x[j], first_y[j]):
            cp.wait_recv()
        for cp in (z_x[j], z_y[j], fwd_x[j], fwd_y[j]):
            cp.start()

    with jax.named_scope('lead_in'):
        relay(1)
        dz_part(e_all, 0, 0, hb, dz00)

    def links_2():
        relay(2)
        for cp in more_x + more_y:
            cp.start()

    def links_6():
        for cp in z_x + fwd_x + fwd_y:
            cp.wait_recv()
        for cp in z_d:
            cp.start()

    def links_11():
        more_y[0].wait_recv()
        last_x.start()

    def arrive(*cps):
        def go():
            for cp in cps:
                cp.wait_recv()
        return go

    actions = {1: arrive(*e_twin), 2: links_2, 3: arrive(*e_rest), 6: links_6, 9: arrive(*z_y), 10: arrive(more_x[0]),
               11: links_11, 12: arrive(z_d[0]), 13: arrive(more_x[1])}

    def act_upon(s, lo, hi):
        for k, act in actions.items():
            if lo <= k < hi:
                @pl.when(s == k)
                def _():
                    with jax.named_scope(f'arr{k}'):
                        act()

    def tok(b, lo=0, n=BLK):
        return pl.ds(pl.multiple_of(b * BLK + lo, 256), n)

    def total(parts):
        out = parts[0]
        for v in parts[1:]:
            out = out + v
        return out

    def group(blks, nxt, last):
        for t in range(N_TASK):
            dz, da = dzs[t % 2], das[t % 2]
            rows = slice(t * sl, (t + 1) * sl)
            for b, u, h in blks:
                da[h][...] = (nn_dot(w2s[...], dz[h][...]) * sl_own[u]).astype(BF16)
            if t < N_TASK - 1:
                for b, u, h in blks:
                    dz_part(e_all, b, t + 1, hb, dzs[(t + 1) % 2][h])
            elif nxt is not None:
                dz_part(e_all, nxt, 0, hb, dzs[0][0])
            g2[rows, :] += total([nt_dot(ut_own[u], dz[h][...]) for b, u, h in blks])
            g1[rows, :] += total([nn_dot(da[h][...], x_all[tok(b), :]) for b, u, h in blks])
            if last and t > 0:
                for cp in (halves[t] if t > 1 else halves[0] + halves[1]):
                    cp.start()

    n_own = ut_own.shape[0]

    def own_body(s, c):
        act_upon(s, 0, n_own)
        group([(s, s, 0)], s + 1, False)
        return c

    def far_body(s, c):
        act_upon(s, n_own, n_blk)
        act_part(x_all[tok(s), :], w1t, ut_own.at[0], sl_own.at[0])
        group([(s, 0, 0)], s + 1, False)
        return c

    with jax.named_scope('main_own'):
        lax.fori_loop(0, n_own, own_body, 0)
    with jax.named_scope('main'):
        lax.fori_loop(n_own, n_blk - 2, far_body, 0)
    with jax.named_scope('last_act'):
        more_y[1].wait_recv()
        z_d[1].wait_recv()
        last_x.wait_recv()
        act_part(x_all[tok(n_blk - 2), :], w1t, ut_own.at[0], sl_own.at[0])
        act_part(x_all[tok(n_blk - 1), :], w1t, ut_own.at[1], sl_own.at[1])
        dz_part(e_all, n_blk - 1, 0, hb, dz01)
    with jax.named_scope('main_last'):
        group([(n_blk - 2, 0, 0), (n_blk - 1, 1, 1)], None, True)

    with jax.named_scope('halves'):
        pairs = [(i, j) for i in range(N_TASK) for j in range(i, N_TASK)]
        acc = tuple(jnp.zeros((8, 128), F32) for _ in pairs)

        def fold(new, old, acc):
            def one(src, dst, n_rows, n_cols, row_of, col0, acc):
                def go(r, acc):
                    row = pl.multiple_of(r * 8, 8)
                    acc = list(acc)
                    for l in range(0, n_cols, 128):
                        gs = {t: dst[t, pl.ds(row, 8), l:l + 128] for t in old}
                        for t in new:
                            v = dst[t, pl.ds(row, 8), l:l + 128] + src[pl.ds(pl.multiple_of(row_of(t) + row, 8), 8),
                                                                       pl.ds(pl.multiple_of(col0 + l, 128), 128)]
                            dst[t, pl.ds(row, 8), l:l + 128] = v
                            gs[t] = v
                        for q, (i, j) in enumerate(pairs):
                            if (i in new or j in new) and i in gs and j in gs:
                                acc[q] = acc[q] + gs[i] * gs[j]
                    return tuple(acc)
                return lax.fori_loop(0, n_rows // 8, go, acc)

            for t in new:
                for cp in halves[t]:
                    cp.wait_recv()
            acc = one(g1, rx1, sl, dim // 2, lambda t: t * sl, keep_col, acc)
            return one(g2, rx2, half, dim, lambda t: t * sl + keep_row, 0, acc)

        acc = fold((0, 1, 2), (), acc)
        acc = fold((3,), (0, 1, 2), acc)
    with jax.named_scope('gram_x'):
        gr_own[...] = jnp.zeros_like(gr_own)
        for q in range(len(pairs)):
            gr_own[q:q + 1, :] = jnp.sum(acc[q], axis=0, keepdims=True)
        loc = pltpu.make_async_copy(gr_own, gr_all.at[me], lsem.at[6])
        loc.start()
        grams = []
        for k in range(1, N_DEV):
            p = lax.rem(me + k, N_DEV)
            grams.append(rcopy(f'gram{k}', gr_own, gr_all.at[me], (p // N_DATA, lax.rem(p, N_DATA))))
            grams[-1].start()

        w_sends = list(wt.values()) + list(w_own.values()) + list(w_peer.values()) + list(wd.values()) + [w_fwd]
        for cp in (w_sends + first_x + first_y + more_x + more_y + fwd_x + fwd_y + [last_x] + z_x + z_y + z_d + e_twin + e_rest
                   + [cp for h in halves for cp in h]):
            cp.wait_send()

        for cp in grams:
            cp.wait()
        loc.wait()
    with jax.named_scope('weights'):
        tot = gr_all[0]
        for k in range(1, N_DEV):
            tot = tot + gr_all[k]
        sums = jnp.broadcast_to(jnp.sum(tot, axis=1, keepdims=True), tot.shape)
        gram = {}
        for q, (i, j) in enumerate(pairs):
            gram[i, j] = gram[j, i] = sums[q:q + 1, :]
        scale = (gram[0, 0] + gram[1, 1] + gram[2, 2] + gram[3, 3]) / N_TASK

        def eg_step(k, w):
            up = []
            for i in range(N_TASK):
                mv = (gram[i, 0] * w[0] + gram[i, 1] * w[1]) + (gram[i, 2] * w[2] + gram[i, 3] * w[3])
                up.append(w[i] * jnp.exp(-mv / scale))
            s = (up[0] + up[1]) + (up[2] + up[3])
            return tuple(u / s for u in up)

        w = lax.fori_loop(0, STEPS, eg_step, tuple(jnp.full((1, 128), 1.0 / N_TASK, F32) for _ in range(N_TASK)))
        wts_ref[...] = jnp.zeros_like(wts_ref)
        for t in range(N_TASK):
            wts_ref[t:t + 1, :] = w[t]
    def blend(rx, l):
        wb = [jnp.broadcast_to(v, (rx.shape[1], 128)) for v in w]
        v = wb[0] * rx[0, :, l:l + 128]
        for t in range(1, N_TASK):
            v = v + wb[t] * rx[t, :, l:l + 128]
        return v

    with jax.named_scope('outs'):
        cols = pl.ds(pl.multiple_of(chip * sl, sl), sl)
        n_dest = N_DATA // 2
        outs = []
        for j in range(n_dest):
            p = n_dest * core + j
            src = tr_ref.at[j * p1:(j + 1) * p1, :]
            outs.append((p, pltpu.make_async_remote_copy(src, rx_g1.at[:, cols], osend.at[j], orecv.at[chip],
                                                         device_id=(m, p), device_id_type=MESH),
                         pltpu.make_async_copy(src, rx_g1.at[:, cols], lsem.at[7])))
        for l in range(0, dim // 2, 128):
            tr_ref[l:l + 128, :] = blend(rx1, l).T
        for p, far, near in outs:
            @pl.when(p != d)
            def _():
                far.start()

            @pl.when(p == d)
            def _():
                near.start()
        for l in range(0, dim, 128):
            out2_ref[:, l:l + 128] = blend(rx2, l)
        for k in range(N_DATA // 2):
            @pl.when(jnp.logical_or(core != d // n_dest, chip != k))
            def _():
                pltpu.make_async_remote_copy(tr_ref.at[0:p1, :], rx_g1.at[:, k * sl:(k + 1) * sl], osend.at[0], orecv.at[k],
                                             device_id=peer, device_id_type=MESH).wait_recv()
        for p, far, near in outs:
            @pl.when(p != d)
            def _():
                far.wait_send()

            @pl.when(p == d)
            def _():
                near.wait()
        out1_ref[...] = rx_g1[...]
    assert len(table) <= ssem.shape[0]


def mega_call(n_total, tokens, w_up, w_down, task_heads, labels):
    n_loc, dim = tokens.shape
    wide = w_up.shape[1]
    sl = 2 * wide // N_DATA
    half = sl // 2
    per = dim // N_DATA
    n_half = n_loc // 2
    vm = pl.BlockSpec(memory_space=pltpu.VMEM)
    hbm = pl.BlockSpec(memory_space=pl.ANY)
    vmem = pltpu.VMEM
    return pl.pallas_call(
        functools.partial(mega_kernel, n_total),
        out_shape=[jax.ShapeDtypeStruct((8, 128), F32), jax.ShapeDtypeStruct((per, half * N_DATA), F32),
                   jax.ShapeDtypeStruct((half, dim), F32)],
        in_specs=[hbm, hbm, hbm, vm, vm],
        out_specs=[vm, vm, vm],
        scratch_shapes=[vmem((4 * n_loc, dim), BF16), vmem((4 * n_loc // BLK, 8, BLK), F32),
                        vmem((dim, wide), BF16), vmem((wide, dim), BF16), vmem((dim, wide), BF16), vmem((wide, dim), BF16),
                        vmem((sl, dim), BF16), vmem((sl, dim), BF16),
                        vmem((N_TASK * (N_CLASS - 1), dim, 128), F32),
                        vmem((2, n_half // 2, dim), F32), vmem((2, n_half // 2, wide), BF16),
                        vmem((N_TASK * sl, dim), F32), vmem((N_TASK * sl, dim), F32),
                        vmem((N_TASK, sl, dim // 2), F32), vmem((N_TASK, half, dim), F32),
                        *[vmem((dim, BLK), BF16)] * 4, *[vmem((sl, BLK), BF16)] * 4, vmem((4, sl, BLK), BF16), vmem((4, sl, BLK), F32),
                        vmem((16, 128), F32), vmem((N_DEV, 16, 128), F32), vmem((dim // 2, sl), F32), vmem((per, wide), F32),
                        pltpu.SemaphoreType.DMA((100,)), pltpu.SemaphoreType.DMA((100,)), pltpu.SemaphoreType.DMA((8,)),
                        pltpu.SemaphoreType.DMA((4,)), pltpu.SemaphoreType.DMA((4,))],
        compiler_params=pltpu.CompilerParams(vmem_limit_bytes=VMEM_LIMIT, collective_id=0, has_side_effects=True),
    )(tokens, w_up, w_down, task_heads, labels)


def final_kernel(wts_in, g1_in, g2_in, wts_ref, g1_ref, g2_ref):
    for t in range(N_TASK):
        wts_ref[t] = wts_in[t, 0]
    g1_ref[...] = g1_in[...]
    g2_ref[...] = g2_in[...]


def final_call(wts, g1, g2):
    vm = pl.BlockSpec(memory_space=pltpu.VMEM)
    return pl.pallas_call(
        final_kernel,
        out_shape=[jax.ShapeDtypeStruct((N_TASK,), F32), jax.ShapeDtypeStruct(g1.shape, F32), jax.ShapeDtypeStruct(g2.shape, F32)],
        in_specs=[vm, vm, vm],
        out_specs=[pl.BlockSpec(memory_space=pltpu.SMEM), vm, vm],
        compiler_params=pltpu.CompilerParams(vmem_limit_bytes=VMEM_LIMIT),
    )(wts, g1, g2)


def solution(mesh):
    n_data = mesh.shape['data']

    def local_step(tokens, w_up, w_down, task_heads, labels):
        wts, up, down = mega_call(tokens.shape[0] * n_data, tokens, w_up, w_down, task_heads.transpose(2, 0, 1), labels)
        return final_call(wts, up, down)

    return jax.shard_map(
        local_step, mesh=mesh,
        in_specs=(P('data', None), P(None, 'model'), P('model', None), P(None, None, None), P(None, 'data')),
        out_specs=(P(None), P('data', 'model'), P(('model', 'data'), None)),
        check_vma=False)
```

```python
import functools

import jax
import jax.numpy as jnp
from jax import lax
from jax.experimental import pallas as pl
from jax.experimental.pallas import tpu as pltpu
from jax.sharding import PartitionSpec as P

STEPS = 20
MESH = pl.DeviceIdType.MESH
F32 = jnp.float32
BF16 = jnp.bfloat16
C0 = 0.7978845608028654
C1 = 0.044715
N_DATA = 8
N_DEV = 16
N_TASK = 4
N_CLASS = 3
BLK = 512
LANE = 128
VMEM_LIMIT = 63 * 1024 * 1024


def gelu_only(a):
    return a * (0.5 + 0.5 * jnp.tanh(a * (C0 + (C0 * C1) * (a * a))))


def gelu_both(a):
    a2 = a * a
    t = jnp.tanh(a * (C0 + (C0 * C1) * a2))
    h = 0.5 + 0.5 * t
    act = a * h
    return act, h + act * (1.0 - h) * (2.0 * C0 + (6.0 * C0 * C1) * a2)


def nt_dot(a, b):
    return lax.dot_general(a, b, (((1,), (1,)), ((), ())), preferred_element_type=F32)


def nn_dot(a, b):
    return jnp.dot(a, b, preferred_element_type=F32)


def xor_data(d, dr):
    core = lax.rem(d, 2)
    x = lax.rem(d // 2, 2)
    y = d // 4
    return (lax.rem(y + dr // 2, 2) * 2 + lax.rem(x + dr % 2, 2)) * 2 + core


def dz_part(e_ref, s, t, hb_ref, dz):
    dim, blk = dz.shape
    rows = 32
    es = [[e_ref[s, N_TASK * c + t:N_TASK * c + t + 1, lo:lo + LANE] for lo in range(0, blk, LANE)] for c in range(N_CLASS - 1)]
    for r0 in range(0, dim, rows):
        h = [hb_ref[(N_CLASS - 1) * t + c, r0:r0 + rows, :] for c in range(N_CLASS - 1)]
        for j in range(blk // LANE):
            val = h[0] * es[0][j] + h[1] * es[1][j]
            dz[r0:r0 + rows, LANE * j:LANE * j + LANE] = val.astype(BF16)


def act_part(x, w1t_ref, ut, sl):
    act, slope = gelu_both(nt_dot(w1t_ref[...], x))
    ut[...] = act.astype(BF16)
    sl[...] = slope


def mega_kernel(n_total, x_hbm, w1_hbm, w2_hbm, heads_hbm, lab_hbm, wts_ref, out1_ref, out2_ref,
                x_all, e_all, w1v, w2v, w1f, w2f, w1t, w2s, hb, part, act_far, g1, g2, rx1, rx2,
                dz00, dz01, dz10, dz11, da00, da01, da10, da11, ut_own, sl_own, gr_own, gr_all, tr_ref, rx_g1, heads_ref, lab_ref,
                ssem, rsem, lsem, osend, orecv):
    m = lax.axis_index('model')
    d = lax.axis_index('data')
    core = lax.rem(d, 2)
    chip = d // 2
    me = m * N_DATA + d
    dim = x_all.shape[1]
    wide = w1v.shape[1]
    sl = w1t.shape[0]
    half = sl // 2
    p1 = dim // N_DATA
    p2 = wide // N_DATA

    def slot(k, lo=0, n=BLK):
        return x_all.at[pl.ds(k * BLK + lo, n), :]

    lcopy = [pltpu.make_async_copy(x_hbm.at[pl.ds(pl.multiple_of((2 * m + k) * BLK, BLK), BLK), :], slot(k), lsem.at[k])
             for k in range(2)]
    lcopy += [pltpu.make_async_copy(w1_hbm, w1v, lsem.at[2]), pltpu.make_async_copy(w2_hbm, w2v, lsem.at[3])]
    lcopy += [pltpu.make_async_copy(x_hbm.at[pl.ds(pl.multiple_of((2 - 2 * m + k) * BLK, BLK), BLK), :], slot(2 + k),
                                    lsem.at[4 + k]) for k in range(2)]
    lcopy += [pltpu.make_async_copy(heads_hbm, heads_ref, lsem.at[8]), pltpu.make_async_copy(lab_hbm, lab_ref, lsem.at[9])]
    for cp in lcopy:
        cp.start()

    barrier = pltpu.get_barrier_semaphore()
    for k in range(1, N_DEV):
        p = lax.rem(me + k, N_DEV)
        pl.semaphore_signal(barrier, inc=1, device_id=(p // N_DATA, lax.rem(p, N_DATA)), device_id_type=MESH)
    pl.semaphore_wait(barrier, N_DEV - 1)

    twin = (1 - m, d)
    peer = (m, d + 1 - 2 * core)
    nb_x = (m, xor_data(d, 1))
    nb_y = (m, xor_data(d, 2))

    table = {}

    def rcopy(name, src, dst, dev):
        if name not in table:
            table[name] = len(table)
        k = table[name]
        return pltpu.make_async_remote_copy(src, dst, ssem.at[k], rsem.at[k], device_id=dev, device_id_type=MESH)

    def w_rows(w, dr, part=None, ref=None):
        n = p1 if w == 1 else p2
        lo, size = (0, n) if part is None else (part * (n // 2), n // 2)
        ref = (w1f if w == 1 else w2f) if ref is None else ref
        return ref.at[pl.ds(pl.multiple_of(xor_data(d, dr) * n + lo, n // 2), size), :]

    w_hbm = {1: w1_hbm, 2: w2_hbm}
    wt = {(w, h): rcopy(f't{w}{h}', w_rows(w, 0, h, w_hbm[w]), w_rows(w, 0, h), twin) for w in (1, 2) for h in (0, 1)}
    wd = {1: rcopy('d1', w_rows(1, 3, 1, w1_hbm), w_rows(1, 3, 1), twin), 2: rcopy('d2', w_rows(2, 3, None, w2_hbm), w_rows(2, 3), twin)}
    w_own = {(w, h, n): rcopy(f'o{w}{h}{n}', w_rows(w, 0, h), w_rows(w, 0, h), dev)
             for w in (1, 2) for h in (0, 1) for n, dev in (('x', nb_x), ('y', nb_y))}
    w_peer = {(w, dr): rcopy(f'p{w}{dr}', w_rows(w, dr), w_rows(w, dr), peer) for w in (1, 2) for dr in range(4)}
    w_fwd = rcopy('g0', w_rows(1, 1, 0), w_rows(1, 1, 0), nb_y)

    pieces = ((0, BLK // 4), (BLK // 4, BLK // 4), (BLK // 2, BLK // 2))

    def own_piece(b, lo, n):
        return x_hbm.at[pl.ds(pl.multiple_of(b * BLK + lo, BLK // 4), n), :]

    def cut(name, src, dst, dev):
        return [rcopy(f'{name}{lo}', slot(src, lo, n), slot(dst, lo, n), dev) for lo, n in pieces]

    first_x = [rcopy(f'fx{lo}', own_piece(3 * m, lo, n), slot(4, lo, n), nb_x) for lo, n in pieces]
    first_y = [rcopy(f'fy{lo}', own_piece(1 + m, lo, n), slot(5, lo, n), nb_y) for lo, n in pieces]
    more_x = [rcopy(f'mx{b}', own_piece(b, 0, BLK), slot(k), nb_x) for b, k in ((1, 10), (2, 13))]
    more_y = [rcopy(f'my{k}', own_piece(b, 0, BLK), slot(k), nb_y) for b, k in ((3 - 3 * m, 11), (3 * m, 14))]
    fwd_x = cut('dx', 5, 7, nb_x)
    fwd_y = cut('dy', 4, 8, nb_y)
    z_x = cut('zx', 4, 6, twin)
    z_y = cut('zy', 5, 9, twin)
    keep15 = BLK - BLK // 4
    z_d = [rcopy('zd7', slot(7), slot(12), twin), rcopy('zd8', slot(8, 0, keep15), slot(15, 0, keep15), twin)]
    last_x = rcopy('lx', slot(11, keep15, BLK // 4), slot(15, keep15, BLK // 4), nb_x)

    k_out, k_in = m, 1 - m
    e_twin = [rcopy(f'et{k}', e_all.at[k], e_all.at[2 + k], twin) for k in range(2)]
    e_rest = []
    for dz in (0, 1):
        for dr in (1, 2, 3):
            dev = (lax.rem(m + dz, 2), xor_data(d, dr))
            s_out, s_in = {1: (4 + 2 * dz, 10 + 3 * m), 2: (14 - 3 * dz, 5 + 4 * dz), 3: (8 + 7 * dz, 7 + 5 * dz)}[dr]
            e_rest.append(rcopy(f'eo{dz}{dr}', e_all.at[k_out], e_all.at[s_out], dev))
            e_rest.append(rcopy(f'ei{dz}{dr}', e_all.at[k_in], e_all.at[s_in], dev))

    wt[1, 0].start()
    wt[1, 1].start()
    first_x[0].start()
    first_y[0].start()
    wt[2, 0].start()
    wt[2, 1].start()
    wd[1].start()
    wd[2].start()
    for k in range(4):
        lcopy[k].wait()

    fc = wide // 3

    def part_block(k):
        x = x_all[k * BLK:(k + 1) * BLK, :]
        acc = None
        for f in range(0, wide, fc):
            u = gelu_only(nn_dot(x, w1v[:, f:f + fc])).astype(BF16)
            y = nn_dot(u, w2v[f:f + fc, :])
            acc = y if acc is None else acc + y
        part[k] = acc

    def act_own(k):
        act_part(x_all[k * BLK:(k + 1) * BLK, :], w1t, ut_own.at[k], sl_own.at[k])

    with jax.named_scope('near'):
        part_block(0)
        for cp in lcopy[6:]:
            cp.wait()
        wt[1, 0].wait_recv()
        for n in 'xy':
            w_own[1, 0, n].start()
        for c in range(N_CLASS - 1):
            h = heads_ref[c].astype(F32) - heads_ref[N_CLASS - 1].astype(F32)
            h = jnp.concatenate([h, h], axis=0).T
            for t in range(N_TASK):
                hb[(N_CLASS - 1) * t + c] = jnp.broadcast_to(h[:, t:t + 1], (dim, LANE))
        off = pl.multiple_of(chip * sl, sl)
        w1t[...] = w1v[:, pl.ds(off, sl)].T
        w2s[...] = w2v[pl.ds(off, sl), :]
        wt[1, 1].wait_recv()
        for n in 'xy':
            w_own[1, 1, n].start()
        w_peer[1, 0].start()
        part_block(1)
    with jax.named_scope('wait_t2'):
        w_own[1, 0, 'x'].wait_recv()
        w_fwd.start()
        wt[2, 0].wait_recv()
        for n in 'xy':
            w_own[2, 0, n].start()
        for n, dr, hs in (('x', 1, (1,)), ('y', 2, (0, 1))):
            for h in hs:
                w_own[1, h, n].wait_recv()
            w_peer[1, dr].start()
        wt[2, 1].wait_recv()
        for n in 'xy':
            w_own[2, 1, n].start()
        w_peer[2, 0].start()
        for j in (1, 2):
            first_x[j].start()
            first_y[j].start()
    for k in (4, 5):
        lcopy[k].wait()
    act_own(0)
    act_own(1)
    first_x[0].wait_recv()
    z_x[0].start()
    first_y[0].wait_recv()
    act_own(2)
    act_own(3)
    with jax.named_scope('wait_w1'):
        w_fwd.wait_recv()
        wd[1].wait_recv()
        w_peer[1, 3].start()
        for h in (0, 1):
            w_own[2, h, 'x'].wait_recv()
        w_peer[2, 1].start()
        for dr in range(4):
            w_peer[1, dr].wait_recv()
    with jax.named_scope('far1'):
        for k in range(2):
            x = x_all[k * BLK:(k + 1) * BLK, :]
            for f in range(0, wide, fc):
                act_far[k, :, f:f + fc] = gelu_only(nn_dot(x, w1f[:, f:f + fc])).astype(BF16)
    def w2_pair(k, j):
        rows = pl.ds(pl.multiple_of(lax.rem(chip // 2 + j, 2) * (2 * sl), 2 * sl), 2 * sl)
        part[k] += nn_dot(act_far[k, :, rows], w2f[rows, :])

    with jax.named_scope('wait_w2'):
        for h in (0, 1):
            w_own[2, h, 'y'].wait_recv()
        w_peer[2, 2].start()
        for dr in (0, 1):
            w_peer[2, dr].wait_recv()
        w2_pair(0, 0)
        wd[2].wait_recv()
        w_peer[2, 3].start()
        g1[...] = jnp.zeros_like(g1)
        g2[...] = jnp.zeros_like(g2)
        w2_pair(1, 0)
        for dr in (2, 3):
            w_peer[2, dr].wait_recv()
    with jax.named_scope('errs'):
        heads16 = jnp.concatenate([heads_ref[c] for c in range(N_CLASS)] + [heads_ref[0]], axis=0)
        for k in range(2):
            w2_pair(k, 1)
            z = (x_all[k * BLK:(k + 1) * BLK, :].astype(F32) + part[k]).astype(BF16)
            logits = nt_dot(heads16, z)
            lg = [logits[N_TASK * c:N_TASK * c + N_TASK, :] for c in range(N_CLASS)]
            top = jnp.maximum(jnp.maximum(lg[0], lg[1]), lg[2])
            ex = [jnp.exp(v - top) for v in lg]
            tot = ex[0] + ex[1] + ex[2]
            lab = lab_ref[:, pl.ds(pl.multiple_of((2 * m + k) * BLK, BLK), BLK)]
            for c in range(N_CLASS - 1):
                rest = (ex[1 - c] + ex[2]) / tot
                e_all[k, N_TASK * c:N_TASK * c + N_TASK, :] = jnp.where(lab == c, -rest, ex[c] / tot) * (1.0 / n_total)
        for cp in e_twin + e_rest:
            cp.start()
        for cp in (z_y[0], fwd_x[0], fwd_y[0]):
            cp.start()

    dzs, das = ((dz00, dz01), (dz10, dz11)), ((da00, da01), (da10, da11))
    n_blk = x_all.shape[0] // BLK
    keep_row = pl.multiple_of(core * half, half)
    give_row = pl.multiple_of((1 - core) * half, half)
    keep_col = pl.multiple_of(core * (dim // 2), LANE)
    give_col = pl.multiple_of((1 - core) * (dim // 2), LANE)
    halves = [(rcopy(f'h1{t}', g1.at[pl.ds(t * sl, sl), pl.ds(give_col, dim // 2)], rx1.at[t], peer),
               rcopy(f'h2{t}', g2.at[pl.ds(t * sl + give_row, half), :], rx2.at[t], peer)) for t in range(N_TASK)]

    def relay(j):
        for cp in (first_x[j], first_y[j]):
            cp.wait_recv()
        for cp in (z_x[j], z_y[j], fwd_x[j], fwd_y[j]):
            cp.start()

    with jax.named_scope('lead_in'):
        relay(1)
        dz_part(e_all, 0, 0, hb, dz00)

    def links_2():
        relay(2)
        for cp in more_x + more_y:
            cp.start()

    def links_7():
        for cp in fwd_x + fwd_y:
            cp.wait_recv()
        for cp in z_d:
            cp.start()

    def links_11():
        more_y[0].wait_recv()
        last_x.start()

    def arrive(*cps):
        def go():
            for cp in cps:
                cp.wait_recv()
        return go

    actions = {1: arrive(*e_twin), 2: links_2, 3: arrive(*e_rest), 6: arrive(*z_x), 7: links_7, 9: arrive(*z_y), 10: arrive(more_x[0]),
               11: links_11, 12: arrive(z_d[0]), 13: arrive(more_x[1])}

    def act_upon(s, lo, hi):
        for k, act in actions.items():
            if lo <= k < hi:
                @pl.when(s == k)
                def _():
                    with jax.named_scope(f'arr{k}'):
                        act()

    def tok(b, lo=0, n=BLK):
        return pl.ds(pl.multiple_of(b * BLK + lo, 256), n)

    def total(parts):
        out = parts[0]
        for v in parts[1:]:
            out = out + v
        return out

    def group(blks, nxt, last):
        for t in range(N_TASK):
            dz, da = dzs[t % 2], das[t % 2]
            rows = slice(t * sl, (t + 1) * sl)
            for b, u, h in blks:
                da[h][...] = (nn_dot(w2s[...], dz[h][...]) * sl_own[u]).astype(BF16)
            if t < N_TASK - 1:
                for b, u, h in blks:
                    dz_part(e_all, b, t + 1, hb, dzs[(t + 1) % 2][h])
            elif nxt is not None:
                dz_part(e_all, nxt, 0, hb, dzs[0][0])
            g2[rows, :] += total([nt_dot(ut_own[u], dz[h][...]) for b, u, h in blks])
            g1[rows, :] += total([nn_dot(da[h][...], x_all[tok(b), :]) for b, u, h in blks])
            if last and t > 0:
                for cp in (halves[t] if t > 1 else halves[0] + halves[1]):
                    cp.start()

    n_own = ut_own.shape[0]

    def own_body(s, c):
        act_upon(s, 0, n_own)
        group([(s, s, 0)], s + 1, False)
        return c

    def far_body(s, c):
        act_upon(s, n_own, n_blk)
        act_part(x_all[tok(s), :], w1t, ut_own.at[0], sl_own.at[0])
        group([(s, 0, 0)], s + 1, False)
        return c

    with jax.named_scope('main_own'):
        lax.fori_loop(0, n_own, own_body, 0)
    with jax.named_scope('main'):
        lax.fori_loop(n_own, n_blk - 2, far_body, 0)
    with jax.named_scope('last_act'):
        more_y[1].wait_recv()
        z_d[1].wait_recv()
        last_x.wait_recv()
        act_part(x_all[tok(n_blk - 2), :], w1t, ut_own.at[0], sl_own.at[0])
        act_part(x_all[tok(n_blk - 1), :], w1t, ut_own.at[1], sl_own.at[1])
        dz_part(e_all, n_blk - 1, 0, hb, dz01)
    with jax.named_scope('main_last'):
        group([(n_blk - 2, 0, 0), (n_blk - 1, 1, 1)], None, True)

    with jax.named_scope('halves'):
        pairs = [(i, j) for i in range(N_TASK) for j in range(i, N_TASK)]
        acc = tuple(jnp.zeros((8, LANE), F32) for _ in pairs)

        def fold(new, old, acc):
            def one(src, dst, n_rows, n_cols, row_of, col0, acc):
                def go(r, acc):
                    row = pl.multiple_of(r * 8, 8)
                    acc = list(acc)
                    for l in range(0, n_cols, LANE):
                        gs = {t: dst[t, pl.ds(row, 8), l:l + LANE] for t in old}
                        for t in new:
                            v = dst[t, pl.ds(row, 8), l:l + LANE] + src[pl.ds(pl.multiple_of(row_of(t) + row, 8), 8),
                                                                       pl.ds(pl.multiple_of(col0 + l, LANE), LANE)]
                            dst[t, pl.ds(row, 8), l:l + LANE] = v
                            gs[t] = v
                        for q, (i, j) in enumerate(pairs):
                            if (i in new or j in new) and i in gs and j in gs:
                                acc[q] = acc[q] + gs[i] * gs[j]
                    return tuple(acc)
                return lax.fori_loop(0, n_rows // 8, go, acc)

            for t in new:
                for cp in halves[t]:
                    cp.wait_recv()
            acc = one(g1, rx1, sl, dim // 2, lambda t: t * sl, keep_col, acc)
            return one(g2, rx2, half, dim, lambda t: t * sl + keep_row, 0, acc)

        acc = fold((0, 1, 2), (), acc)
        acc = fold((3,), (0, 1, 2), acc)
    with jax.named_scope('gram_x'):
        gr_own[...] = jnp.zeros_like(gr_own)
        for q in range(len(pairs)):
            gr_own[q:q + 1, :] = jnp.sum(acc[q], axis=0, keepdims=True)
        loc = pltpu.make_async_copy(gr_own, gr_all.at[me], lsem.at[6])
        loc.start()
        grams = []
        for k in range(1, N_DEV):
            p = lax.rem(me + k, N_DEV)
            grams.append(rcopy(f'gram{k}', gr_own, gr_all.at[me], (p // N_DATA, lax.rem(p, N_DATA))))
            grams[-1].start()

        w_sends = list(wt.values()) + list(w_own.values()) + list(w_peer.values()) + list(wd.values()) + [w_fwd]
        for cp in (w_sends + first_x + first_y + more_x + more_y + fwd_x + fwd_y + [last_x] + z_x + z_y + z_d + e_twin + e_rest
                   + [cp for h in halves for cp in h]):
            cp.wait_send()

        for cp in grams:
            cp.wait()
        loc.wait()
    with jax.named_scope('weights'):
        tot = gr_all[0]
        for k in range(1, N_DEV):
            tot = tot + gr_all[k]
        sums = jnp.broadcast_to(jnp.sum(tot, axis=1, keepdims=True), tot.shape)
        gram = {}
        for q, (i, j) in enumerate(pairs):
            gram[i, j] = gram[j, i] = sums[q:q + 1, :]
        scale = total([gram[i, i] for i in range(N_TASK)]) / N_TASK

        def eg_step(k, w):
            up = []
            for i in range(N_TASK):
                mv = (gram[i, 0] * w[0] + gram[i, 1] * w[1]) + (gram[i, 2] * w[2] + gram[i, 3] * w[3])
                up.append(w[i] * jnp.exp(-mv / scale))
            s = (up[0] + up[1]) + (up[2] + up[3])
            return tuple(u / s for u in up)

        w = lax.fori_loop(0, STEPS, eg_step, tuple(jnp.full((1, LANE), 1.0 / N_TASK, F32) for _ in range(N_TASK)))
        wts_ref[...] = jnp.zeros_like(wts_ref)
        for t in range(N_TASK):
            wts_ref[t:t + 1, :] = w[t]
    def blend(rx, l):
        wb = [jnp.broadcast_to(v, (rx.shape[1], LANE)) for v in w]
        v = wb[0] * rx[0, :, l:l + LANE]
        for t in range(1, N_TASK):
            v = v + wb[t] * rx[t, :, l:l + LANE]
        return v

    with jax.named_scope('outs'):
        cols = pl.ds(pl.multiple_of(chip * sl, sl), sl)
        n_dest = N_DATA // 2
        outs = []
        for j in range(n_dest):
            p = n_dest * core + j
            src = tr_ref.at[j * p1:(j + 1) * p1, :]
            outs.append((p, pltpu.make_async_remote_copy(src, rx_g1.at[:, cols], osend.at[j], orecv.at[chip],
                                                         device_id=(m, p), device_id_type=MESH),
                         pltpu.make_async_copy(src, rx_g1.at[:, cols], lsem.at[7])))
        for l in range(0, dim // 2, LANE):
            tr_ref[l:l + LANE, :] = blend(rx1, l).T
        for p, far, near in outs:
            @pl.when(p != d)
            def _():
                far.start()

            @pl.when(p == d)
            def _():
                near.start()
        for l in range(0, dim, LANE):
            out2_ref[:, l:l + LANE] = blend(rx2, l)
        for k in range(N_DATA // 2):
            @pl.when(jnp.logical_or(core != d // n_dest, chip != k))
            def _():
                pltpu.make_async_remote_copy(tr_ref.at[0:p1, :], rx_g1.at[:, k * sl:(k + 1) * sl], osend.at[0], orecv.at[k],
                                             device_id=peer, device_id_type=MESH).wait_recv()
        for p, far, near in outs:
            @pl.when(p != d)
            def _():
                far.wait_send()

            @pl.when(p == d)
            def _():
                near.wait()
        out1_ref[...] = rx_g1[...]
    assert len(table) <= ssem.shape[0]


def mega_call(n_total, tokens, w_up, w_down, task_heads, labels):
    n_loc, dim = tokens.shape
    wide = w_up.shape[1]
    sl = 2 * wide // N_DATA
    half = sl // 2
    per = dim // N_DATA
    n_half = n_loc // 2
    vm = pl.BlockSpec(memory_space=pltpu.VMEM)
    hbm = pl.BlockSpec(memory_space=pl.ANY)
    vmem = pltpu.VMEM
    return pl.pallas_call(
        functools.partial(mega_kernel, n_total),
        out_shape=[jax.ShapeDtypeStruct((8, LANE), F32), jax.ShapeDtypeStruct((per, half * N_DATA), F32),
                   jax.ShapeDtypeStruct((half, dim), F32)],
        in_specs=[hbm] * 5,
        out_specs=[vm, vm, vm],
        scratch_shapes=[vmem((4 * n_loc, dim), BF16), vmem((4 * n_loc // BLK, 8, BLK), F32),
                        vmem((dim, wide), BF16), vmem((wide, dim), BF16), vmem((dim, wide), BF16), vmem((wide, dim), BF16),
                        vmem((sl, dim), BF16), vmem((sl, dim), BF16),
                        vmem((N_TASK * (N_CLASS - 1), dim, LANE), F32),
                        vmem((2, n_half // 2, dim), F32), vmem((2, n_half // 2, wide), BF16),
                        vmem((N_TASK * sl, dim), F32), vmem((N_TASK * sl, dim), F32),
                        vmem((N_TASK, sl, dim // 2), F32), vmem((N_TASK, half, dim), F32),
                        *[vmem((dim, BLK), BF16)] * 4, *[vmem((sl, BLK), BF16)] * 4, vmem((4, sl, BLK), BF16), vmem((4, sl, BLK), F32),
                        vmem((16, LANE), F32), vmem((N_DEV, 16, LANE), F32), vmem((dim // 2, sl), F32), vmem((per, wide), F32),
                        vmem(task_heads.shape, BF16), vmem(labels.shape, jnp.int32),
                        pltpu.SemaphoreType.DMA((100,)), pltpu.SemaphoreType.DMA((100,)), pltpu.SemaphoreType.DMA((10,)),
                        pltpu.SemaphoreType.DMA((4,)), pltpu.SemaphoreType.DMA((4,))],
        compiler_params=pltpu.CompilerParams(vmem_limit_bytes=VMEM_LIMIT, collective_id=0, has_side_effects=True),
    )(tokens, w_up, w_down, task_heads, labels)


def final_kernel(wts_in, g1_in, g2_in, wts_ref, g1_ref, g2_ref):
    for t in range(N_TASK):
        wts_ref[t] = wts_in[t, 0]
    g1_ref[...] = g1_in[...]
    g2_ref[...] = g2_in[...]


def final_call(wts, g1, g2):
    vm = pl.BlockSpec(memory_space=pltpu.VMEM)
    return pl.pallas_call(
        final_kernel,
        out_shape=[jax.ShapeDtypeStruct((N_TASK,), F32), jax.ShapeDtypeStruct(g1.shape, F32), jax.ShapeDtypeStruct(g2.shape, F32)],
        in_specs=[vm, vm, vm],
        out_specs=[pl.BlockSpec(memory_space=pltpu.SMEM), vm, vm],
        compiler_params=pltpu.CompilerParams(vmem_limit_bytes=VMEM_LIMIT),
    )(wts, g1, g2)


def solution(mesh):
    n_data = mesh.shape['data']

    def local_step(tokens, w_up, w_down, task_heads, labels):
        wts, up, down = mega_call(tokens.shape[0] * n_data, tokens, w_up, w_down, task_heads.transpose(2, 0, 1), labels)
        return final_call(wts, up, down)

    return jax.shard_map(
        local_step, mesh=mesh,
        in_specs=(P('data', None), P(None, 'model'), P('model', None), P(None, None, None), P(None, 'data')),
        out_specs=(P(None), P('data', 'model'), P(('model', 'data'), None)),
        check_vma=False)
```

```python
import functools

import jax
import jax.numpy as jnp
from jax import lax
from jax.experimental import pallas as pl
from jax.experimental.pallas import tpu as pltpu
from jax.sharding import PartitionSpec as P

STEPS = 20
MESH = pl.DeviceIdType.MESH
F32 = jnp.float32
BF16 = jnp.bfloat16
C0 = 0.7978845608028654
C1 = 0.044715
N_DATA = 8
N_DEV = 16
N_TASK = 4
N_CLASS = 3
BLK = 512
LANE = 128
VMEM_LIMIT = 63 * 1024 * 1024


def gelu_only(a):
    return a * (0.5 + 0.5 * jnp.tanh(a * (C0 + (C0 * C1) * (a * a))))


def gelu_both(a):
    a2 = a * a
    t = jnp.tanh(a * (C0 + (C0 * C1) * a2))
    h = 0.5 + 0.5 * t
    act = a * h
    return act, h + act * (1.0 - h) * (2.0 * C0 + (6.0 * C0 * C1) * a2)


def nt_dot(a, b):
    return lax.dot_general(a, b, (((1,), (1,)), ((), ())), preferred_element_type=F32)


def nn_dot(a, b):
    return jnp.dot(a, b, preferred_element_type=F32)


def xor_data(d, dr):
    core = lax.rem(d, 2)
    x = lax.rem(d // 2, 2)
    y = d // 4
    return (lax.rem(y + dr // 2, 2) * 2 + lax.rem(x + dr % 2, 2)) * 2 + core


def dz_part(e_ref, s, t, hb_ref, dz):
    dim, blk = dz.shape
    rows = 32
    es = [[e_ref[s, N_TASK * c + t:N_TASK * c + t + 1, lo:lo + LANE] for lo in range(0, blk, LANE)] for c in range(N_CLASS - 1)]
    for r0 in range(0, dim, rows):
        h = [hb_ref[(N_CLASS - 1) * t + c, r0:r0 + rows, :] for c in range(N_CLASS - 1)]
        for j in range(blk // LANE):
            val = h[0] * es[0][j] + h[1] * es[1][j]
            dz[r0:r0 + rows, LANE * j:LANE * j + LANE] = val.astype(BF16)


def act_part(x, w1t_ref, ut, sl):
    act, slope = gelu_both(nt_dot(w1t_ref[...], x))
    ut[...] = act.astype(BF16)
    sl[...] = slope


def mega_kernel(n_total, x_hbm, w1_hbm, w2_hbm, heads_hbm, lab_hbm, wts_ref, out1_ref, out2_ref,
                x_all, e_all, w1v, w2v, w1f, w2f, w1t, w2s, hb, part, act_far, g1, g2, rx1, rx2,
                dz00, dz01, dz10, dz11, da00, da01, da10, da11, ut_own, sl_own, gr_own, gr_all, tr_ref, rx_g1, heads_ref, lab_ref,
                ssem, rsem, lsem, osend, orecv):
    m = lax.axis_index('model')
    d = lax.axis_index('data')
    core = lax.rem(d, 2)
    chip = d // 2
    me = m * N_DATA + d
    dim = x_all.shape[1]
    wide = w1v.shape[1]
    sl = w1t.shape[0]
    half = sl // 2
    p1 = dim // N_DATA
    p2 = wide // N_DATA

    def slot(k, lo=0, n=BLK):
        return x_all.at[pl.ds(k * BLK + lo, n), :]

    lcopy = [pltpu.make_async_copy(x_hbm.at[pl.ds(pl.multiple_of((2 * m + k) * BLK, BLK), BLK), :], slot(k), lsem.at[k])
             for k in range(2)]
    lcopy += [pltpu.make_async_copy(w1_hbm, w1v, lsem.at[2]), pltpu.make_async_copy(w2_hbm, w2v, lsem.at[3])]
    lcopy += [pltpu.make_async_copy(x_hbm.at[pl.ds(pl.multiple_of((2 - 2 * m + k) * BLK, BLK), BLK), :], slot(2 + k),
                                    lsem.at[4 + k]) for k in range(2)]
    lcopy += [pltpu.make_async_copy(heads_hbm, heads_ref, lsem.at[8]), pltpu.make_async_copy(lab_hbm, lab_ref, lsem.at[9])]
    for cp in lcopy:
        cp.start()

    barrier = pltpu.get_barrier_semaphore()
    for k in range(1, N_DEV):
        p = lax.rem(me + k, N_DEV)
        pl.semaphore_signal(barrier, inc=1, device_id=(p // N_DATA, lax.rem(p, N_DATA)), device_id_type=MESH)
    pl.semaphore_wait(barrier, N_DEV - 1)

    twin = (1 - m, d)
    peer = (m, d + 1 - 2 * core)
    nb_x = (m, xor_data(d, 1))
    nb_y = (m, xor_data(d, 2))

    table = {}

    def rcopy(name, src, dst, dev):
        if name not in table:
            table[name] = len(table)
        k = table[name]
        return pltpu.make_async_remote_copy(src, dst, ssem.at[k], rsem.at[k], device_id=dev, device_id_type=MESH)

    def w_rows(w, dr, part=None, ref=None):
        n = p1 if w == 1 else p2
        lo, size = (0, n) if part is None else (part * (n // 2), n // 2)
        ref = (w1f if w == 1 else w2f) if ref is None else ref
        return ref.at[pl.ds(pl.multiple_of(xor_data(d, dr) * n + lo, n // 2), size), :]

    w_hbm = {1: w1_hbm, 2: w2_hbm}
    wt = {(w, h): rcopy(f't{w}{h}', w_rows(w, 0, h, w_hbm[w]), w_rows(w, 0, h), twin) for w in (1, 2) for h in (0, 1)}
    wd = {1: rcopy('d1', w_rows(1, 3, 1, w1_hbm), w_rows(1, 3, 1), twin), 2: rcopy('d2', w_rows(2, 3, None, w2_hbm), w_rows(2, 3), twin)}
    w_own = {(w, h, n): rcopy(f'o{w}{h}{n}', w_rows(w, 0, h), w_rows(w, 0, h), dev)
             for w in (1, 2) for h in (0, 1) for n, dev in (('x', nb_x), ('y', nb_y))}
    w_peer = {(w, dr): rcopy(f'p{w}{dr}', w_rows(w, dr), w_rows(w, dr), peer) for w in (1, 2) for dr in range(4)}
    w_fwd = rcopy('g0', w_rows(1, 1, 0), w_rows(1, 1, 0), nb_y)

    lead = 5 * BLK // 16
    pieces = ((0, lead), (lead, BLK // 2 - lead), (BLK // 2, BLK // 2))

    def own_piece(b, lo, n):
        return x_hbm.at[pl.ds(pl.multiple_of(b * BLK + lo, BLK // 16), n), :]

    def cut(name, src, dst, dev):
        return [rcopy(f'{name}{lo}', slot(src, lo, n), slot(dst, lo, n), dev) for lo, n in pieces]

    first_x = [rcopy(f'fx{lo}', own_piece(3 * m, lo, n), slot(4, lo, n), nb_x) for lo, n in pieces]
    first_y = [rcopy(f'fy{lo}', own_piece(1 + m, lo, n), slot(5, lo, n), nb_y) for lo, n in pieces]
    more_x = [rcopy(f'mx{b}', own_piece(b, 0, BLK), slot(k), nb_x) for b, k in ((1, 10), (2, 13))]
    more_y = [rcopy(f'my{k}', own_piece(b, 0, BLK), slot(k), nb_y) for b, k in ((3 - 3 * m, 11), (3 * m, 14))]
    fwd_x = cut('dx', 5, 7, nb_x)
    fwd_y = cut('dy', 4, 8, nb_y)
    z_x = cut('zx', 4, 6, twin)
    z_y = cut('zy', 5, 9, twin)
    keep15 = BLK - lead
    z_d = [rcopy('zd7', slot(7), slot(12), twin), rcopy('zd8', slot(8, 0, keep15), slot(15, 0, keep15), twin)]
    last_x = rcopy('lx', slot(11, keep15, lead), slot(15, keep15, lead), nb_x)

    k_out, k_in = m, 1 - m
    e_twin = [rcopy(f'et{k}', e_all.at[k], e_all.at[2 + k], twin) for k in range(2)]
    e_rest = []
    for dz in (0, 1):
        for dr in (1, 2, 3):
            dev = (lax.rem(m + dz, 2), xor_data(d, dr))
            s_out, s_in = {1: (4 + 2 * dz, 10 + 3 * m), 2: (14 - 3 * dz, 5 + 4 * dz), 3: (8 + 7 * dz, 7 + 5 * dz)}[dr]
            e_rest.append(rcopy(f'eo{dz}{dr}', e_all.at[k_out], e_all.at[s_out], dev))
            e_rest.append(rcopy(f'ei{dz}{dr}', e_all.at[k_in], e_all.at[s_in], dev))

    wt[1, 0].start()
    wt[1, 1].start()
    first_x[0].start()
    first_y[0].start()
    wt[2, 0].start()
    wt[2, 1].start()
    wd[1].start()
    wd[2].start()
    for k in range(4):
        lcopy[k].wait()

    fc = wide // 3

    def part_block(k):
        x = x_all[k * BLK:(k + 1) * BLK, :]
        acc = None
        for f in range(0, wide, fc):
            u = gelu_only(nn_dot(x, w1v[:, f:f + fc])).astype(BF16)
            y = nn_dot(u, w2v[f:f + fc, :])
            acc = y if acc is None else acc + y
        part[k] = acc

    def act_own(k):
        act_part(x_all[k * BLK:(k + 1) * BLK, :], w1t, ut_own.at[k], sl_own.at[k])

    with jax.named_scope('near'):
        part_block(0)
        for cp in lcopy[6:]:
            cp.wait()
        wt[1, 0].wait_recv()
        for n in 'xy':
            w_own[1, 0, n].start()
        for c in range(N_CLASS - 1):
            h = heads_ref[c].astype(F32) - heads_ref[N_CLASS - 1].astype(F32)
            h = jnp.concatenate([h, h], axis=0).T
            for t in range(N_TASK):
                hb[(N_CLASS - 1) * t + c] = jnp.broadcast_to(h[:, t:t + 1], (dim, LANE))
        off = pl.multiple_of(chip * sl, sl)
        w1t[...] = w1v[:, pl.ds(off, sl)].T
        w2s[...] = w2v[pl.ds(off, sl), :]
        wt[1, 1].wait_recv()
        for n in 'xy':
            w_own[1, 1, n].start()
        w_peer[1, 0].start()
        part_block(1)
    with jax.named_scope('wait_t2'):
        w_own[1, 0, 'x'].wait_recv()
        w_fwd.start()
        wt[2, 0].wait_recv()
        for n in 'xy':
            w_own[2, 0, n].start()
        for n, dr, hs in (('x', 1, (1,)), ('y', 2, (0, 1))):
            for h in hs:
                w_own[1, h, n].wait_recv()
            w_peer[1, dr].start()
        wt[2, 1].wait_recv()
        for n in 'xy':
            w_own[2, 1, n].start()
        w_peer[2, 0].start()
        for j in (1, 2):
            first_x[j].start()
            first_y[j].start()
    for k in (4, 5):
        lcopy[k].wait()
    act_own(0)
    act_own(1)
    first_x[0].wait_recv()
    z_x[0].start()
    first_y[0].wait_recv()
    act_own(2)
    act_own(3)
    with jax.named_scope('wait_w1'):
        w_fwd.wait_recv()
        wd[1].wait_recv()
        w_peer[1, 3].start()
        for h in (0, 1):
            w_own[2, h, 'x'].wait_recv()
        w_peer[2, 1].start()
        for dr in range(4):
            w_peer[1, dr].wait_recv()
    with jax.named_scope('far1'):
        for k in range(2):
            x = x_all[k * BLK:(k + 1) * BLK, :]
            for f in range(0, wide, fc):
                act_far[k, :, f:f + fc] = gelu_only(nn_dot(x, w1f[:, f:f + fc])).astype(BF16)
    def w2_pair(k, j):
        rows = pl.ds(pl.multiple_of(lax.rem(chip // 2 + j, 2) * (2 * sl), 2 * sl), 2 * sl)
        part[k] += nn_dot(act_far[k, :, rows], w2f[rows, :])

    with jax.named_scope('wait_w2'):
        for h in (0, 1):
            w_own[2, h, 'y'].wait_recv()
        w_peer[2, 2].start()
        for dr in (0, 1):
            w_peer[2, dr].wait_recv()
        w2_pair(0, 0)
        wd[2].wait_recv()
        w_peer[2, 3].start()
        g1[...] = jnp.zeros_like(g1)
        g2[...] = jnp.zeros_like(g2)
        w2_pair(1, 0)
        for dr in (2, 3):
            w_peer[2, dr].wait_recv()
    with jax.named_scope('errs'):
        heads16 = jnp.concatenate([heads_ref[c] for c in range(N_CLASS)] + [heads_ref[0]], axis=0)
        for k in range(2):
            w2_pair(k, 1)
            z = (x_all[k * BLK:(k + 1) * BLK, :].astype(F32) + part[k]).astype(BF16)
            logits = nt_dot(heads16, z)
            lg = [logits[N_TASK * c:N_TASK * c + N_TASK, :] for c in range(N_CLASS)]
            top = jnp.maximum(jnp.maximum(lg[0], lg[1]), lg[2])
            ex = [jnp.exp(v - top) for v in lg]
            tot = ex[0] + ex[1] + ex[2]
            lab = lab_ref[:, pl.ds(pl.multiple_of((2 * m + k) * BLK, BLK), BLK)]
            for c in range(N_CLASS - 1):
                rest = (ex[1 - c] + ex[2]) / tot
                e_all[k, N_TASK * c:N_TASK * c + N_TASK, :] = jnp.where(lab == c, -rest, ex[c] / tot) * (1.0 / n_total)
        for cp in e_twin + e_rest:
            cp.start()
        for cp in (z_y[0], fwd_x[0], fwd_y[0]):
            cp.start()

    dzs, das = ((dz00, dz01), (dz10, dz11)), ((da00, da01), (da10, da11))
    n_blk = x_all.shape[0] // BLK
    keep_row = pl.multiple_of(core * half, half)
    give_row = pl.multiple_of((1 - core) * half, half)
    keep_col = pl.multiple_of(core * (dim // 2), LANE)
    give_col = pl.multiple_of((1 - core) * (dim // 2), LANE)
    halves = [(rcopy(f'h1{t}', g1.at[pl.ds(t * sl, sl), pl.ds(give_col, dim // 2)], rx1.at[t], peer),
               rcopy(f'h2{t}', g2.at[pl.ds(t * sl + give_row, half), :], rx2.at[t], peer)) for t in range(N_TASK)]

    def relay(j):
        for cp in (first_x[j], first_y[j]):
            cp.wait_recv()
        for cp in (z_x[j], fwd_x[j], fwd_y[j]):
            cp.start()

    with jax.named_scope('lead_in'):
        relay(1)
        dz_part(e_all, 0, 0, hb, dz00)

    def links_2():
        relay(2)
        for cp in z_y[1:] + more_x + more_y:
            cp.start()

    def links_7():
        for cp in fwd_x + fwd_y:
            cp.wait_recv()
        for cp in z_d:
            cp.start()

    def links_11():
        more_y[0].wait_recv()
        last_x.start()

    def arrive(*cps):
        def go():
            for cp in cps:
                cp.wait_recv()
        return go

    actions = {1: arrive(*e_twin), 2: links_2, 3: arrive(*e_rest), 6: arrive(*z_x), 7: links_7, 9: arrive(*z_y), 10: arrive(more_x[0]),
               11: links_11, 12: arrive(z_d[0]), 13: arrive(more_x[1])}

    def act_upon(s, lo, hi):
        for k, act in actions.items():
            if lo <= k < hi:
                @pl.when(s == k)
                def _():
                    with jax.named_scope(f'arr{k}'):
                        act()

    def tok(b, lo=0, n=BLK):
        return pl.ds(pl.multiple_of(b * BLK + lo, 256), n)

    def total(parts):
        out = parts[0]
        for v in parts[1:]:
            out = out + v
        return out

    def group(blks, nxt, last):
        for t in range(N_TASK):
            dz, da = dzs[t % 2], das[t % 2]
            rows = slice(t * sl, (t + 1) * sl)
            for b, u, h in blks:
                da[h][...] = (nn_dot(w2s[...], dz[h][...]) * sl_own[u]).astype(BF16)
            if t < N_TASK - 1:
                for b, u, h in blks:
                    dz_part(e_all, b, t + 1, hb, dzs[(t + 1) % 2][h])
            elif nxt is not None:
                dz_part(e_all, nxt, 0, hb, dzs[0][0])
            g2[rows, :] += total([nt_dot(ut_own[u], dz[h][...]) for b, u, h in blks])
            if last and t == N_TASK - 1:
                halves[t][1].start()
            g1[rows, :] += total([nn_dot(da[h][...], x_all[tok(b), :]) for b, u, h in blks])
            if last and t > 0:
                for cp in (halves[0] + halves[1], halves[2], halves[3][:1])[t - 1]:
                    cp.start()

    n_own = ut_own.shape[0]

    def own_body(s, c):
        act_upon(s, 0, n_own)
        group([(s, s, 0)], s + 1, False)
        return c

    def far_body(s, c):
        act_upon(s, n_own, n_blk)
        act_part(x_all[tok(s), :], w1t, ut_own.at[0], sl_own.at[0])
        group([(s, 0, 0)], s + 1, False)
        return c

    with jax.named_scope('main_own'):
        lax.fori_loop(0, n_own, own_body, 0)
    with jax.named_scope('main'):
        lax.fori_loop(n_own, n_blk - 2, far_body, 0)
    with jax.named_scope('last_act'):
        more_y[1].wait_recv()
        act_part(x_all[tok(n_blk - 2), :], w1t, ut_own.at[0], sl_own.at[0])
        z_d[1].wait_recv()
        last_x.wait_recv()
        act_part(x_all[tok(n_blk - 1), :], w1t, ut_own.at[1], sl_own.at[1])
        dz_part(e_all, n_blk - 1, 0, hb, dz01)
    with jax.named_scope('main_last'):
        group([(n_blk - 2, 0, 0), (n_blk - 1, 1, 1)], None, True)

    with jax.named_scope('halves'):
        pairs = [(i, j) for i in range(N_TASK) for j in range(i, N_TASK)]
        acc = tuple(jnp.zeros((8, LANE), F32) for _ in pairs)

        def fold(new, old, acc):
            def one(src, dst, n_rows, n_cols, row_of, col0, acc):
                def go(r, acc):
                    row = pl.multiple_of(r * 8, 8)
                    acc = list(acc)
                    for l in range(0, n_cols, LANE):
                        gs = {t: dst[t, pl.ds(row, 8), l:l + LANE] for t in old}
                        for t in new:
                            v = dst[t, pl.ds(row, 8), l:l + LANE] + src[pl.ds(pl.multiple_of(row_of(t) + row, 8), 8),
                                                                       pl.ds(pl.multiple_of(col0 + l, LANE), LANE)]
                            dst[t, pl.ds(row, 8), l:l + LANE] = v
                            gs[t] = v
                        for q, (i, j) in enumerate(pairs):
                            if (i in new or j in new) and i in gs and j in gs:
                                acc[q] = acc[q] + gs[i] * gs[j]
                    return tuple(acc)
                return lax.fori_loop(0, n_rows // 8, go, acc)

            for t in new:
                for cp in halves[t]:
                    cp.wait_recv()
            acc = one(g1, rx1, sl, dim // 2, lambda t: t * sl, keep_col, acc)
            return one(g2, rx2, half, dim, lambda t: t * sl + keep_row, 0, acc)

        acc = fold((0, 1, 2), (), acc)
        acc = fold((3,), (0, 1, 2), acc)
    with jax.named_scope('gram_x'):
        gr_own[...] = jnp.zeros_like(gr_own)
        for q in range(len(pairs)):
            gr_own[q:q + 1, :] = jnp.sum(acc[q], axis=0, keepdims=True)
        loc = pltpu.make_async_copy(gr_own, gr_all.at[me], lsem.at[6])
        loc.start()
        grams = []
        for k in range(1, N_DEV):
            p = lax.rem(me + k, N_DEV)
            grams.append(rcopy(f'gram{k}', gr_own, gr_all.at[me], (p // N_DATA, lax.rem(p, N_DATA))))
            grams[-1].start()

        w_sends = list(wt.values()) + list(w_own.values()) + list(w_peer.values()) + list(wd.values()) + [w_fwd]
        for cp in (w_sends + first_x + first_y + more_x + more_y + fwd_x + fwd_y + [last_x] + z_x + z_y + z_d + e_twin + e_rest
                   + [cp for h in halves for cp in h]):
            cp.wait_send()

        for cp in grams:
            cp.wait()
        loc.wait()
    with jax.named_scope('weights'):
        tot = gr_all[0]
        for k in range(1, N_DEV):
            tot = tot + gr_all[k]
        sums = jnp.broadcast_to(jnp.sum(tot, axis=1, keepdims=True), tot.shape)
        gram = {}
        for q, (i, j) in enumerate(pairs):
            gram[i, j] = gram[j, i] = sums[q:q + 1, :]
        scale = total([gram[i, i] for i in range(N_TASK)]) / N_TASK

        def eg_step(k, w):
            up = []
            for i in range(N_TASK):
                mv = (gram[i, 0] * w[0] + gram[i, 1] * w[1]) + (gram[i, 2] * w[2] + gram[i, 3] * w[3])
                up.append(w[i] * jnp.exp(-mv / scale))
            s = (up[0] + up[1]) + (up[2] + up[3])
            return tuple(u / s for u in up)

        w = lax.fori_loop(0, STEPS, eg_step, tuple(jnp.full((1, LANE), 1.0 / N_TASK, F32) for _ in range(N_TASK)))
        wts_ref[...] = jnp.zeros_like(wts_ref)
        for t in range(N_TASK):
            wts_ref[t:t + 1, :] = w[t]
    def blend(rx, l):
        wb = [jnp.broadcast_to(v, (rx.shape[1], LANE)) for v in w]
        v = wb[0] * rx[0, :, l:l + LANE]
        for t in range(1, N_TASK):
            v = v + wb[t] * rx[t, :, l:l + LANE]
        return v

    with jax.named_scope('outs'):
        cols = pl.ds(pl.multiple_of(chip * sl, sl), sl)
        n_dest = N_DATA // 2
        outs = []
        for j in range(n_dest):
            p = n_dest * core + j
            src = tr_ref.at[j * p1:(j + 1) * p1, :]
            outs.append((p, pltpu.make_async_remote_copy(src, rx_g1.at[:, cols], osend.at[j], orecv.at[chip],
                                                         device_id=(m, p), device_id_type=MESH),
                         pltpu.make_async_copy(src, rx_g1.at[:, cols], lsem.at[7])))
        for l in range(0, dim // 2, LANE):
            tr_ref[l:l + LANE, :] = blend(rx1, l).T
        for p, far, near in outs:
            @pl.when(p != d)
            def _():
                far.start()

            @pl.when(p == d)
            def _():
                near.start()
        for l in range(0, dim, LANE):
            out2_ref[:, l:l + LANE] = blend(rx2, l)
        for k in range(N_DATA // 2):
            @pl.when(jnp.logical_or(core != d // n_dest, chip != k))
            def _():
                pltpu.make_async_remote_copy(tr_ref.at[0:p1, :], rx_g1.at[:, k * sl:(k + 1) * sl], osend.at[0], orecv.at[k],
                                             device_id=peer, device_id_type=MESH).wait_recv()
        for p, far, near in outs:
            @pl.when(p != d)
            def _():
                far.wait_send()

            @pl.when(p == d)
            def _():
                near.wait()
        out1_ref[...] = rx_g1[...]
    assert len(table) <= ssem.shape[0]


def mega_call(n_total, tokens, w_up, w_down, task_heads, labels):
    n_loc, dim = tokens.shape
    wide = w_up.shape[1]
    sl = 2 * wide // N_DATA
    half = sl // 2
    per = dim // N_DATA
    n_half = n_loc // 2
    vm = pl.BlockSpec(memory_space=pltpu.VMEM)
    hbm = pl.BlockSpec(memory_space=pl.ANY)
    vmem = pltpu.VMEM
    return pl.pallas_call(
        functools.partial(mega_kernel, n_total),
        out_shape=[jax.ShapeDtypeStruct((8, LANE), F32), jax.ShapeDtypeStruct((per, half * N_DATA), F32),
                   jax.ShapeDtypeStruct((half, dim), F32)],
        in_specs=[hbm] * 5,
        out_specs=[vm, vm, vm],
        scratch_shapes=[vmem((4 * n_loc, dim), BF16), vmem((4 * n_loc // BLK, 8, BLK), F32),
                        vmem((dim, wide), BF16), vmem((wide, dim), BF16), vmem((dim, wide), BF16), vmem((wide, dim), BF16),
                        vmem((sl, dim), BF16), vmem((sl, dim), BF16),
                        vmem((N_TASK * (N_CLASS - 1), dim, LANE), F32),
                        vmem((2, n_half // 2, dim), F32), vmem((2, n_half // 2, wide), BF16),
                        vmem((N_TASK * sl, dim), F32), vmem((N_TASK * sl, dim), F32),
                        vmem((N_TASK, sl, dim // 2), F32), vmem((N_TASK, half, dim), F32),
                        *[vmem((dim, BLK), BF16)] * 4, *[vmem((sl, BLK), BF16)] * 4, vmem((4, sl, BLK), BF16), vmem((4, sl, BLK), F32),
                        vmem((16, LANE), F32), vmem((N_DEV, 16, LANE), F32), vmem((dim // 2, sl), F32), vmem((per, wide), F32),
                        vmem(task_heads.shape, BF16), vmem(labels.shape, jnp.int32),
                        pltpu.SemaphoreType.DMA((100,)), pltpu.SemaphoreType.DMA((100,)), pltpu.SemaphoreType.DMA((10,)),
                        pltpu.SemaphoreType.DMA((4,)), pltpu.SemaphoreType.DMA((4,))],
        compiler_params=pltpu.CompilerParams(vmem_limit_bytes=VMEM_LIMIT, collective_id=0, has_side_effects=True),
    )(tokens, w_up, w_down, task_heads, labels)


def final_kernel(wts_in, g1_in, g2_in, wts_ref, g1_ref, g2_ref):
    for t in range(N_TASK):
        wts_ref[t] = wts_in[t, 0]
    g1_ref[...] = g1_in[...]
    g2_ref[...] = g2_in[...]


def final_call(wts, g1, g2):
    vm = pl.BlockSpec(memory_space=pltpu.VMEM)
    return pl.pallas_call(
        final_kernel,
        out_shape=[jax.ShapeDtypeStruct((N_TASK,), F32), jax.ShapeDtypeStruct(g1.shape, F32), jax.ShapeDtypeStruct(g2.shape, F32)],
        in_specs=[vm, vm, vm],
        out_specs=[pl.BlockSpec(memory_space=pltpu.SMEM), vm, vm],
        compiler_params=pltpu.CompilerParams(vmem_limit_bytes=VMEM_LIMIT),
    )(wts, g1, g2)


def solution(mesh):
    n_data = mesh.shape['data']

    def local_step(tokens, w_up, w_down, task_heads, labels):
        wts, up, down = mega_call(tokens.shape[0] * n_data, tokens, w_up, w_down, task_heads.transpose(2, 0, 1), labels)
        return final_call(wts, up, down)

    return jax.shard_map(
        local_step, mesh=mesh,
        in_specs=(P('data', None), P(None, 'model'), P('model', None), P(None, None, None), P(None, 'data')),
        out_specs=(P(None), P('data', 'model'), P(('model', 'data'), None)),
        check_vma=False)
```
